128 devices in a mesh: dom: 128 (over y, z, x, core).
Axes of the slice: x: 4, y: 4, z: 4, core: 2. Of those that a mesh axis runs over, the one named last changes fastest.
Arguments:
- right_side: float32 [131072, 3], P('dom'), may hold values from -10 to 10
- fine_diagonal: float32 [131072, 3], P('dom'), may hold values from 2 to 4
- fine_columns: int32 [131072, 27], P('dom'), may hold values from 0 to 131071, as said below
- fine_blocks: float32 [131072, 27, 3, 3], P('dom'), may hold values from -0.625 to 0.625
- aggregate_of_node: int32 [131072], P('dom'), may hold values from 0 to 31, as said below
- coarse_row_of_aggregate: int32 [4096], P('dom'), may hold values from 0 to 4095, as said below
- coarse_diagonal: float32 [4096, 3], P('dom'), may hold values from 2 to 4
- coarse_columns: int32 [4096, 27], P('dom'), may hold values from 0 to 4095
- coarse_blocks: float32 [4096, 27, 3, 3], P('dom'), may hold values from -0.625 to 0.625
Outputs:
- solution: float32 [131072, 3], P('dom')
- correction: float32 [4096, 3], P('dom')
The draws below stay inside these ranges and needn't reach their ends.
Inputs may be any that keep to these rules, and one draw needn't show every extreme that they name: Every entry of fine_columns differs from its row number by at most 256, and some entry by exactly 256. `aggregate_of_node`: on each device every aggregate number 0 to 31 is used by at least one of its nodes. coarse_row_of_aggregate is a permutation of 0 to 4095; among the 32 aggregates of one device (an aligned block of entries) at most 8 get rows of any one owner, and exactly 8 for some owner.
All inputs are finite; a program needn't handle non-finite values.
Results may differ from the reference program's by a relative error of at most 0.0003.
Values sent between devices are 32-bit elements.
A program may use at most 64 MiB of HBM per device.

```python
import jax
import jax.numpy as jnp
from jax import lax

NODE_DEV = 1024
CAP = 8
WIN = 256
NNZ = 27
CNNZ = 27
SWEEPS = 2
CSWEEPS = 6
AGG_DEV = 32
NODES = 131072
AGGS = 4096


def draw_fine_columns(key, part):
    row_ids = jnp.arange(NODES, dtype=jnp.int32)[:, None]
    offset = jax.random.randint(jax.random.fold_in(key, 13), (NODES, NNZ), -WIN, WIN + 1)
    columns = jnp.clip(row_ids + offset, 0, NODES - 1)
    return columns.at[0, 0].set(WIN).astype(jnp.int32)


def draw_aggregate_of_node(key, part):
    devices = NODES // NODE_DEV
    key_raw, key_mix = jax.random.split(jax.random.fold_in(key, 11))
    labels_raw = jax.random.randint(key_raw, (devices, NODE_DEV), 0, AGG_DEV)
    labels_raw = labels_raw.at[:, :AGG_DEV].set(jnp.arange(AGG_DEV, dtype=jnp.int32)[None, :])
    mixers = jax.random.split(key_mix, devices)
    shuffles = jax.vmap(lambda one_key: jax.random.permutation(one_key, NODE_DEV))(mixers)
    return jnp.take_along_axis(labels_raw, shuffles, axis=1).reshape(-1).astype(jnp.int32)


def draw_coarse_row_of_aggregate(key, part):
    devices = AGGS // AGG_DEV
    groups = AGG_DEV // CAP
    key_group, key_slot, key_label = jax.random.split(jax.random.fold_in(key, 17), 3)
    scores = jax.random.permutation(key_group, devices).astype(jnp.int32)
    scores = scores.at[devices // 2].set(-3).at[1].set(-2).at[devices - 1].set(-1)
    offsets = jnp.argsort(scores, stable=True)[:groups].astype(jnp.int32)
    sources = jnp.arange(devices, dtype=jnp.int32)[:, None]
    label_mix = jax.vmap(lambda one_key: jax.random.permutation(one_key, AGG_DEV))(jax.random.split(key_label, devices)).astype(jnp.int32)
    group_ids = label_mix // CAP
    owners = (sources + offsets[group_ids]) % devices
    within = group_ids * CAP + label_mix % CAP
    slot_mix = jax.vmap(lambda one_key: jax.random.permutation(one_key, AGG_DEV))(jax.random.split(key_slot, devices)).astype(jnp.int32)
    slots = slot_mix[owners, within]
    return (owners * AGG_DEV + slots).reshape(-1).astype(jnp.int32)


def with_ends(drawn, own_key, low, high):
    spot = [jax.random.randint(jax.random.fold_in(own_key, axis), (), 0, length) for axis, length in enumerate(drawn.shape)]
    main_axis = drawn.shape.index(max(drawn.shape))
    neighbour = spot[:main_axis] + [(spot[main_axis] + 1) % drawn.shape[main_axis]] + spot[main_axis + 1:]
    return drawn.at[tuple(spot)].set(low).at[tuple(neighbour)].set(high)


def level_of(own_key, extent, cuts, low, high):
    loudness, own = 1.0, jax.random.fold_in(own_key, 6)
    for dim, blocks in cuts:
        draws = jnp.exp(jax.random.uniform(jax.random.fold_in(own, dim), (blocks,), jnp.float32, low / len(cuts), high / len(cuts)))
        loudness = loudness * jnp.repeat(draws, extent[dim] // blocks).reshape([-1 if axis == dim else 1 for axis in range(len(extent))])
    return loudness


def bell_draw(key, shape, scale, reach, cuts=(), kind=jnp.bfloat16):
    gain = level_of(key, shape, cuts, -0.22, 0.18) if cuts else 1.0
    values = jax.random.normal(key, shape, jnp.float32) * scale * gain
    return jnp.minimum(jnp.maximum(values, -reach), reach).astype(kind)


def setup_inputs(seed: int = 0) -> dict:
    seeds = jax.random.split(jax.random.key(seed), 10)
    return {
        "right_side": bell_draw(seeds[0], (NODES, 3), 2.0, 10.0, ((0, 128),), jnp.float32),
        "fine_diagonal": jnp.clip(2.0 + 2.0 * jax.random.uniform(seeds[1], (NODES, 3), jnp.float32) ** level_of(seeds[1], (NODES, 3), ((0, 128),), -0.2, 0.2), 2.0, 4.0),
        "fine_columns": draw_fine_columns(jax.random.fold_in(seeds[9], 71), 0),
        "fine_blocks": bell_draw(seeds[3], (NODES, NNZ, 3, 3), (3 * NNZ) ** -0.5, 0.625, ((0, 128),), jnp.float32),
        "aggregate_of_node": draw_aggregate_of_node(jax.random.fold_in(seeds[9], 71), 0),
        "coarse_row_of_aggregate": draw_coarse_row_of_aggregate(jax.random.fold_in(seeds[9], 71), 0),
        "coarse_diagonal": jnp.clip(2.0 + 2.0 * jax.random.uniform(seeds[6], (AGGS, 3), jnp.float32) ** level_of(seeds[6], (AGGS, 3), ((0, 128),), -0.2, 0.2), 2.0, 4.0),
        "coarse_columns": with_ends(jax.random.randint(seeds[7], (AGGS, CNNZ), 0, AGGS), jax.random.fold_in(seeds[7], 1), 0, AGGS - 1).astype(jnp.int32),
        "coarse_blocks": bell_draw(seeds[8], (AGGS, CNNZ, 3, 3), (3 * CNNZ) ** -0.5, 0.625, ((0, 128),), jnp.float32),
    }


damping = 0.7


def apply_level(field, diagonal, columns, blocks):
    nearby = field[columns]
    pulled = jnp.einsum("rkij,rkj->ri", blocks, nearby, precision=lax.Precision.HIGHEST)
    return diagonal * field - pulled


def reference(right_side, fine_diagonal, fine_columns, fine_blocks, aggregate_of_node, coarse_row_of_aggregate, coarse_diagonal, coarse_columns, coarse_blocks):
    solution = jnp.zeros_like(right_side)
    for sweep in range(SWEEPS):
        solution = solution + damping * (right_side - apply_level(solution, fine_diagonal, fine_columns, fine_blocks)) / fine_diagonal
    residual = right_side - apply_level(solution, fine_diagonal, fine_columns, fine_blocks)
    node_ids = jnp.arange(NODES, dtype=jnp.int32)
    labels = (node_ids // NODE_DEV) * AGG_DEV + aggregate_of_node
    coarse_rows = coarse_row_of_aggregate[labels]
    coarse_rhs = jax.ops.segment_sum(residual, coarse_rows, num_segments=AGGS)
    correction = jnp.zeros_like(coarse_rhs)
    for sweep in range(CSWEEPS):
        correction = correction + damping * (coarse_rhs - apply_level(correction, coarse_diagonal, coarse_columns, coarse_blocks)) / coarse_diagonal
    solution = solution + correction[coarse_rows]
    for sweep in range(SWEEPS):
        solution = solution + damping * (right_side - apply_level(solution, fine_diagonal, fine_columns, fine_blocks)) / fine_diagonal
    return solution, correction
```

```python
import jax
import jax.numpy as jnp
from jax import lax
from jax.experimental import pallas as pl
from jax.experimental.pallas import tpu as pltpu
from jax.sharding import PartitionSpec as P

DEVICES = 128
NODE_DEV = 1024
WIN = 256
NNZ = 27
AGG_DEV = 32
CSWEEPS = 6
LANES = 128
BLOCKS = NODE_DEV // LANES
SIDE = WIN // LANES
REACH = 2 * SIDE + 1
CUBE = 16
GROUPS = 8
CROWS = 32
DAMP = 0.7
KEEP = 1.0 - DAMP
CUBE_BITS = (0, 1, 3, 5)
GROUP_BITS = (2, 4, 6)
MESH = pl.DeviceIdType.MESH
F32, I32, BF16 = jnp.float32, jnp.int32, jnp.bfloat16


def position_of(row):
    def bit(p):
        return (row >> p) & 1

    high = bit(10) * 16 + bit(8) * 8 + bit(6) * 4 + bit(5) * 2 + bit(11)
    lane = bit(9) * 64 + bit(7) * 32 + (row & 31)
    return high * LANES + lane


def spread(row):
    return jnp.broadcast_to(row, (8, LANES))


def pick(row, lane):
    return jnp.take_along_axis(spread(row), lane, axis=1, mode="promise_in_bounds")


def gather_rows(place, rows, count):
    high, lane = place >> 7, place & 127
    values = [None] * 3
    for r in range(count):
        hit = high == r
        for c in range(3):
            taken = pick(rows(r, c), lane)
            values[c] = taken if r == 0 else jnp.where(hit, taken, values[c])
    return values


def kernel(
    b_h, d_h, q_h, a_h, agg_h, row_h, cd_h, cq_h, ca_h,
    sol_o, cor_o,
    b_v, d_v, q_v, a_v, agg_v, row_v, cd_v, cq_v, ca_v,
    w_v, s1_v, q_s, y_v, r_v, onehot, idx_v,
    f1, hl1, hr1, f2, hl2, hr2, f3, f4, hl4, hr4,
    stage, e0a, e0b, s1a, s1b,
    pack, rm, mx, mp,
    inv_v, dt_v, cbuf,
    load_sem, halo_send, halo_recv, far_send, far_recv, sweep_send, sweep_recv,
):
    me = lax.axis_index("dom")

    def bit(p):
        return (me // (1 << p)) % 2

    member = bit(5) * 8 + bit(3) * 4 + bit(1) * 2 + bit(0)
    group = bit(6) * 4 + bit(4) * 2 + bit(2)
    group_low, group_high = bit(4) * 2 + bit(2), bit(6)

    def flipped(bits, k):
        other = me
        for n, p in enumerate(bits):
            if (k >> n) & 1:
                other = other + (1 - 2 * bit(p)) * (1 << p)
        return other

    cube_peers = [flipped(CUBE_BITS, k) for k in range(1, CUBE)]
    group_peers = [flipped(GROUP_BITS, k) for k in range(1, GROUPS)]
    left, right = (me + DEVICES - 1) % DEVICES, (me + 1) % DEVICES

    loads = []
    for n, (src, dst) in enumerate(
        (
            (b_h, b_v), (d_h, d_v), (agg_h, agg_v), (row_h, row_v), (cd_h, cd_v),
            (cq_h, cq_v), (ca_h, ca_v), (q_h, q_v), (a_h, a_v),
        )
    ):
        copy = pltpu.make_async_copy(src, dst, load_sem.at[n])
        copy.start()
        loads.append(copy)

    barrier = pltpu.get_barrier_semaphore()
    for peer in cube_peers + group_peers + [left, right]:
        pl.semaphore_signal(barrier, inc=1, device_id=(peer,), device_id_type=MESH)

    def send(src, dst, send_sem, recv_sem, peer):
        pltpu.make_async_remote_copy(
            src_ref=src, dst_ref=dst, send_sem=send_sem, recv_sem=recv_sem,
            device_id=(peer,), device_id_type=MESH,
        ).start()

    def wait_bytes(ref, sem):
        pltpu.make_async_copy(ref, ref, sem).wait()

    lane = lax.broadcasted_iota(I32, (1, LANES), 1)
    mine = (lane // AGG_DEV) == group_low

    stage[...] = jnp.zeros_like(stage)
    pack[...] = jnp.zeros_like(pack)
    for n in range(7):
        loads[n].wait()
    w_v[...] = DAMP / d_v[...]
    s1_v[...] = w_v[...] * b_v[...]
    f1[pl.ds(0, 3), :] = s1_v[...]
    place_row = position_of(row_v[...])
    stage[pl.ds(0, 3), pl.ds(0, AGG_DEV)] = cd_v[...]
    stage[pl.ds(3, 1), pl.ds(0, AGG_DEV)] = place_row.astype(F32)
    own = stage[...]
    node_place = pick(own[3:4, :], agg_v[...])
    for n in range(BLOCKS):
        f1[pl.ds(3, 1), pl.ds(n * LANES, LANES)] = node_place[n : n + 1, :]
    own = own + pltpu.roll(own, 32, 1) + pltpu.roll(own, 64, 1) + pltpu.roll(own, 96, 1)
    e0a[group] = jnp.where(mine, own, 0.0)
    for e in range(9):
        pack[e // 4, pl.ds(32 * (e % 4), 32), pl.ds(0, NNZ)] = ca_v[e // 3, e % 3]
    pack[2, pl.ds(32, 32), pl.ds(0, NNZ)] = position_of(cq_v[...]).astype(F32)
    for n in range(3):
        rm[group, pl.ds(32 * n, 32), :] = pack[n].T[0:32, :]

    pl.semaphore_wait(barrier, CUBE - 1 + GROUPS - 1 + 2)

    def send_halo(n, own_ref, from_left, from_right):
        send(own_ref.at[:, pl.ds(NODE_DEV - WIN, WIN)], from_left, halo_send.at[n, 0], halo_recv.at[n, 0], right)
        send(own_ref.at[:, pl.ds(0, WIN)], from_right, halo_send.at[n, 1], halo_recv.at[n, 1], left)

    def wait_halo(n, from_left, from_right):
        wait_bytes(from_left, halo_recv.at[n, 0])
        wait_bytes(from_right, halo_recv.at[n, 1])

    def send_group(n, ref):
        for peer in group_peers:
            send(ref.at[group], ref.at[group], far_send.at[n], far_recv.at[n], peer)

    def send_cube(ref, send_sem, recv_sem):
        for peer in cube_peers:
            send(ref.at[member], ref.at[member], send_sem, recv_sem, peer)

    send_halo(0, f1, hl1, hr1)
    send_group(0, e0a)
    send_group(1, rm)

    loads[7].wait()
    q_s[pl.ds(24, 8), :] = jnp.zeros((8, NODE_DEV), I32)
    base = me * NODE_DEV - WIN
    for n in range(BLOCKS):
        cols = pl.ds(n * LANES, LANES)
        q_s[pl.ds(0, NNZ), cols] = q_v[:, cols] - (base + n * LANES)
    for n in range(BLOCKS):
        label = lax.broadcasted_iota(I32, (LANES, LANES), 0) % AGG_DEV
        onehot[:, pl.ds(n * LANES, LANES)] = (agg_v[pl.ds(n, 1), :] == label).astype(F32).astype(BF16)
    r_v[...] = jnp.zeros_like(r_v)
    loads[8].wait()

    def three(own_ref, from_left, from_right):
        def rows(c, n):
            if n < SIDE:
                return from_left[pl.ds(c, 1), pl.ds(n * LANES, LANES)]
            if n < SIDE + BLOCKS:
                return own_ref[pl.ds(c, 1), pl.ds((n - SIDE) * LANES, LANES)]
            return from_right[pl.ds(c, 1), pl.ds((n - SIDE - BLOCKS) * LANES, LANES)]

        return rows

    def couple_fine(rows):
        for n in range(BLOCKS):
            cols = pl.ds(n * LANES, LANES)
            sums = [None] * 3
            for k in range(4):
                near = gather_rows(q_s[pl.ds(8 * k, 8), cols], lambda r, c: rows(c, n + r), REACH)
                width = min(8, NNZ - 8 * k)
                for i in range(3):
                    term = None
                    for c in range(3):
                        part = a_v[i, c, pl.ds(8 * k, width), cols] * near[c][:width]
                        term = part if term is None else term + part
                    term = jnp.sum(term, axis=0, keepdims=True) if width < 8 else term
                    if k == 0:
                        sums[i] = term
                    elif width == 8:
                        sums[i] = sums[i] + term
                    else:
                        sums[i] = jnp.sum(sums[i], axis=0, keepdims=True) + term
            for i in range(3):
                y_v[pl.ds(i, 1), cols] = sums[i]

    wait_halo(0, hl1, hr1)
    couple_fine(three(f1, hl1, hr1))
    f2[...] = (1.0 + KEEP) * s1_v[...] + w_v[...] * y_v[...]
    send_halo(1, f2, hl2, hr2)

    for n in range(SIDE):
        idx_v[pl.ds(n, 1), :] = hl1[pl.ds(3, 1), pl.ds(n * LANES, LANES)].astype(I32)
        idx_v[pl.ds(SIDE + BLOCKS + n, 1), :] = hr1[pl.ds(3, 1), pl.ds(n * LANES, LANES)].astype(I32)
    for n in range(BLOCKS):
        idx_v[pl.ds(SIDE + n, 1), :] = f1[pl.ds(3, 1), pl.ds(n * LANES, LANES)].astype(I32)
    idx_v[pl.ds(12, 4), :] = jnp.zeros((4, LANES), I32)

    def fold(src, dst):
        for h in range(2):
            dst[member, pl.ds(4 * h, 4), :] = src[4 * h] + src[4 * h + 1] + src[4 * h + 2] + src[4 * h + 3]

    wait_bytes(e0a.at[pl.ds(0, GROUPS - 1)], far_recv.at[0])
    fold(e0a, e0b)
    send_cube(e0b, far_send.at[2], far_recv.at[2])

    wait_bytes(rm.at[pl.ds(0, GROUPS - 1)], far_recv.at[1])
    for h in range(2):
        for e4 in range(3):
            for k in range(4):
                parts = [rm[4 * h + j, pl.ds(32 * e4 + 8 * k, 8), :] for j in range(4)]
                for s in range(4):
                    e = 4 * e4 + s
                    if e > 9:
                        continue
                    whole = None
                    for j in range(4):
                        moved = parts[j] if j == s else pltpu.roll(parts[j], 32 * ((j - s) % 4), 1)
                        whole = moved if j == 0 else jnp.where((lane // 32) == j, moved, whole)
                    rows, cols = pl.ds(8 * k, 8), pl.ds(LANES * h, LANES)
                    if e < 9:
                        mx[e, rows, cols] = whole
                    else:
                        mp[rows, cols] = whole.astype(I32)

    wait_halo(1, hl2, hr2)
    couple_fine(three(f2, hl2, hr2))
    r_v[pl.ds(0, 3), :] = b_v[...] - d_v[...] * f2[...] + y_v[...]
    rest = r_v[...]
    p0 = rest.astype(BF16).astype(F32)
    rest = rest - p0
    p1 = rest.astype(BF16).astype(F32)
    pieces = jnp.concatenate([p0, p1, rest - p1], axis=0).astype(BF16)
    sums = lax.dot_general(pieces, onehot[...], (((1,), (1,)), ((), ())), preferred_element_type=F32)
    sums = sums[0:4] + sums[8:12] + sums[16:20]
    s1a[group] = jnp.where(mine, sums, 0.0)
    send_group(3, s1a)

    wait_bytes(e0b.at[pl.ds(0, CUBE - 1)], far_recv.at[2])
    inverse = None
    for r in range(CROWS):
        place = e0b[r // 2, pl.ds(4 * (r % 2) + 3, 1), :].astype(I32)
        high, low = place >> 7, place & 127
        at_high = lax.broadcasted_iota(I32, (CROWS, LANES), 0) == high
        at_low = (lax.broadcasted_iota(I32, (LANES, LANES), 0) == low).astype(F32).astype(BF16)
        weights = jnp.concatenate(
            [
                jnp.where(at_high, jnp.float32(r), 0.0),
                jnp.where(at_high, lane.astype(F32), 0.0),
            ],
            axis=0,
        ).astype(BF16)
        term = lax.dot_general(weights, at_low, (((1,), (1,)), ((), ())), preferred_element_type=F32)
        inverse = term if inverse is None else inverse + term
    inv_v[...] = (inverse[0:CROWS] * LANES + inverse[CROWS : 2 * CROWS]).astype(I32)
    for r in range(CROWS):
        for c in range(3):
            dt_v[c, pl.ds(r, 1), :] = e0b[r // 2, pl.ds(4 * (r % 2) + c, 1), :]
    for c in range(3):
        dt_v[c] = DAMP / dt_v[c]

    wait_bytes(s1a.at[pl.ds(0, GROUPS - 1)], far_recv.at[3])
    fold(s1a, s1b)
    send_cube(s1b, far_send.at[4], far_recv.at[4])
    wait_bytes(s1b.at[pl.ds(0, CUBE - 1)], far_recv.at[4])

    for t in range(CROWS // 8):
        sums = gather_rows(inv_v[pl.ds(8 * t, 8), :], lambda r, c: s1b[r // 2, pl.ds(4 * (r % 2) + c, 1), :], CROWS)
        for c in range(3):
            value = sums[c] * dt_v[c, pl.ds(8 * t, 8), :]
            for n in range(8):
                r = 8 * t + n
                cbuf[0, r // 2, pl.ds(4 * (r % 2) + c, 1), :] = value[n : n + 1, :]

    unused = lax.broadcasted_iota(I32, (8, LANES), 0) % 4 == 3
    first = jnp.where(unused, 0.0, cbuf[0, member])
    weight = jnp.where(unused, 0.0, DAMP / e0b[member])

    def sweep(n, current):
        totals = []
        for h in range(2):
            cols = pl.ds(LANES * h, LANES)
            sums = [None] * 3
            for k in range(4):
                rows = pl.ds(8 * k, 8)
                near = gather_rows(mp[rows, cols], lambda r, c: cbuf[n, r // 2, pl.ds(4 * (r % 2) + c, 1), :], CROWS)
                for i in range(3):
                    for c in range(3):
                        part = mx[3 * i + c, rows, cols] * near[c]
                        sums[i] = part if sums[i] is None else sums[i] + part
            totals += [jnp.sum(s, axis=0, keepdims=True) for s in sums]
            totals.append(jnp.zeros((1, LANES), F32))
        current = KEEP * current + first + weight * jnp.concatenate(totals, axis=0)
        cbuf[n + 1, member] = current
        send_cube(cbuf.at[n + 1], sweep_send.at[n], sweep_recv.at[n])
        wait_bytes(cbuf.at[n + 1, pl.ds(0, CUBE - 1)], sweep_recv.at[n])
        return current

    last = lax.fori_loop(0, CSWEEPS - 1, sweep, first)

    for t in range(2):
        value = gather_rows(
            idx_v[pl.ds(8 * t, 8), :], lambda r, c: cbuf[CSWEEPS - 1, r // 2, pl.ds(4 * (r % 2) + c, 1), :], CROWS
        )
        rows = three(f2, hl2, hr2)
        for n in range(8 if t == 0 else 4):
            for c in range(3):
                f3[pl.ds(c, 1), pl.ds((8 * t + n) * LANES, LANES)] = rows(c, 8 * t + n) + value[c][n : n + 1, :]
    couple_fine(lambda c, n: f3[pl.ds(c, 1), pl.ds(n * LANES, LANES)])
    f4[...] = KEEP * f3[:, pl.ds(WIN, NODE_DEV)] + s1_v[...] + w_v[...] * y_v[...]
    send_halo(2, f4, hl4, hr4)

    half = jnp.where(group_high == 0, last[0:4], last[4:8])
    moved = half
    for k in range(1, 4):
        moved = jnp.where(group_low == k, pltpu.roll(half, LANES - 32 * k, 1), moved)
    cor_o[...] = moved[0:3, 0:AGG_DEV]

    wait_halo(2, hl4, hr4)
    couple_fine(three(f4, hl4, hr4))
    sol_o[...] = KEEP * f4[...] + s1_v[...] + w_v[...] * y_v[...]

    for n, from_left in enumerate((hl1, hl2, hl4)):
        wait_bytes(from_left, halo_send.at[n, 0])
        wait_bytes(from_left, halo_send.at[n, 1])
    for n, (ref, count) in enumerate(((e0a, GROUPS), (rm, GROUPS), (e0b, CUBE), (s1a, GROUPS), (s1b, CUBE))):
        wait_bytes(ref.at[pl.ds(0, count - 1)], far_send.at[n])
    for n in range(CSWEEPS - 1):
        wait_bytes(cbuf.at[n + 1, pl.ds(0, CUBE - 1)], sweep_send.at[n])


def body(b, d, q, a, agg, row, cd, cq, ca):
    any_spec = pl.BlockSpec(memory_space=pl.ANY)
    vmem = pl.BlockSpec(memory_space=pltpu.VMEM)
    dma = pltpu.SemaphoreType.DMA
    sol, cor = pl.pallas_call(
        kernel,
        out_shape=(
            jax.ShapeDtypeStruct((3, NODE_DEV), F32),
            jax.ShapeDtypeStruct((3, AGG_DEV), F32),
        ),
        in_specs=[any_spec] * 9,
        out_specs=(vmem, vmem),
        scratch_shapes=[
            pltpu.VMEM((3, NODE_DEV), F32),
            pltpu.VMEM((3, NODE_DEV), F32),
            pltpu.VMEM((NNZ, NODE_DEV), I32),
            pltpu.VMEM((3, 3, NNZ, NODE_DEV), F32),
            pltpu.VMEM((BLOCKS, LANES), I32),
            pltpu.VMEM((1, AGG_DEV), I32),
            pltpu.VMEM((3, AGG_DEV), F32),
            pltpu.VMEM((AGG_DEV, NNZ), I32),
            pltpu.VMEM((3, 3, AGG_DEV, NNZ), F32),
            pltpu.VMEM((3, NODE_DEV), F32),
            pltpu.VMEM((3, NODE_DEV), F32),
            pltpu.VMEM((32, NODE_DEV), I32),
            pltpu.VMEM((3, NODE_DEV), F32),
            pltpu.VMEM((8, NODE_DEV), F32),
            pltpu.VMEM((LANES, NODE_DEV), BF16),
            pltpu.VMEM((16, LANES), I32),
            pltpu.VMEM((4, NODE_DEV), F32),
            pltpu.VMEM((4, WIN), F32),
            pltpu.VMEM((4, WIN), F32),
            pltpu.VMEM((3, NODE_DEV), F32),
            pltpu.VMEM((3, WIN), F32),
            pltpu.VMEM((3, WIN), F32),
            pltpu.VMEM((3, NODE_DEV + 2 * WIN), F32),
            pltpu.VMEM((3, NODE_DEV), F32),
            pltpu.VMEM((3, WIN), F32),
            pltpu.VMEM((3, WIN), F32),
            pltpu.VMEM((4, LANES), F32),
            pltpu.VMEM((GROUPS, 4, LANES), F32),
            pltpu.VMEM((CUBE, 8, LANES), F32),
            pltpu.VMEM((GROUPS, 4, LANES), F32),
            pltpu.VMEM((CUBE, 8, LANES), F32),
            pltpu.VMEM((3, LANES, LANES), F32),
            pltpu.VMEM((GROUPS, 96, LANES), F32),
            pltpu.VMEM((9, 32, 2 * LANES), F32),
            pltpu.VMEM((32, 2 * LANES), I32),
            pltpu.VMEM((CROWS, LANES), I32),
            pltpu.VMEM((3, CROWS, LANES), F32),
            pltpu.VMEM((CSWEEPS, CUBE, 8, LANES), F32),
            dma((9,)),
            dma((3, 2)),
            dma((3, 2)),
            dma((5,)),
            dma((5,)),
            dma((CSWEEPS - 1,)),
            dma((CSWEEPS - 1,)),
        ],
        compiler_params=pltpu.CompilerParams(collective_id=0, has_side_effects=True),
        name="vcycle",
    )(
        b.T,
        d.T,
        q.T,
        a.transpose(2, 3, 1, 0),
        agg.reshape(BLOCKS, LANES),
        row.reshape(1, AGG_DEV),
        cd.T,
        cq,
        ca.transpose(2, 3, 0, 1),
    )
    return sol.T, cor.T


def solution(mesh):
    rows, line = P("dom", None), P("dom")
    blocks = P("dom", None, None, None)
    return jax.shard_map(
        body,
        mesh=mesh,
        in_specs=(rows, rows, rows, blocks, line, line, rows, rows, blocks),
        out_specs=(rows, rows),
        check_vma=False,
    )
```

```python
import jax
import jax.numpy as jnp
from jax import lax
from jax.experimental import pallas as pl
from jax.experimental.pallas import tpu as pltpu
from jax.sharding import PartitionSpec as P

DEVICES = 128
NODE_DEV = 1024
WIN = 256
NNZ = 27
AGG_DEV = 32
CSWEEPS = 6
LANES = 128
BLOCKS = NODE_DEV // LANES
SIDE = WIN // LANES
REACH = 2 * SIDE + 1
CUBE = 16
GROUPS = 8
CROWS = 32
DAMP = 0.7
KEEP = 1.0 - DAMP
CUBE_BITS = (0, 1, 3, 5)
GROUP_BITS = (2, 4, 6)
MESH = pl.DeviceIdType.MESH
F32, I32, BF16 = jnp.float32, jnp.int32, jnp.bfloat16


def position_of(row):
    def bit(p):
        return (row >> p) & 1

    high = bit(10) * 16 + bit(8) * 8 + bit(6) * 4 + bit(5) * 2 + bit(11)
    lane = bit(9) * 64 + bit(7) * 32 + (row & 31)
    return high * LANES + lane


def spread(row):
    return jnp.broadcast_to(row, (8, LANES))


def pick(row, lane):
    return jnp.take_along_axis(spread(row), lane, axis=1, mode="promise_in_bounds")


def gather_rows(place, rows, count):
    high, lane = place >> 7, place & 127
    values = [None] * 3
    for r in range(count):
        hit = high == r
        for c in range(3):
            taken = pick(rows(r, c), lane)
            values[c] = taken if r == 0 else jnp.where(hit, taken, values[c])
    return values


def kernel(
    b_h, d_h, q_h, a_h, agg_h, row_h, cd_h, cq_h, ca_h,
    sol_o, cor_o,
    b_v, d_v, q_v, a_v, agg_v, row_v, cd_v, cq_v, ca_v,
    w_v, s1_v, q_s, y_v, r_v, onehot, idx_v,
    f1, hl1, hr1, f2, hl2, hr2, f3, f4, hl4, hr4,
    stage, far0, far1, tab0, tab1,
    pack, rm, mx, mp,
    inv_v, wbuf, cbuf,
    load_sem, halo_send, halo_recv, far_send, far_recv, sweep_send, sweep_recv,
):
    me = lax.axis_index("dom")

    def bit(p):
        return (me // (1 << p)) % 2

    member = bit(5) * 8 + bit(3) * 4 + bit(1) * 2 + bit(0)
    group = bit(6) * 4 + bit(4) * 2 + bit(2)
    group_low, group_high = bit(4) * 2 + bit(2), bit(6)

    def flipped(bits, k):
        other = me
        for n, p in enumerate(bits):
            if (k >> n) & 1:
                other = other + (1 - 2 * bit(p)) * (1 << p)
        return other

    def ring(low, high):
        at = bit(high) * 2 + bit(low)
        places = [(at + k) % 4 for k in range(4)]
        return [(v // 2) * (1 << high) + (v % 2) * (1 << low) for v in places]

    along_x, along_z, along_y = ring(1, 2), ring(3, 4), ring(5, 6)
    cores = [bit(0), 1 - bit(0)]
    steps = [(x, z, y, c) for x in range(4) for z in range(4) for y in range(4) for c in range(2)]
    hops = (0, 1, 2, 1)
    steps = sorted(steps, key=lambda v: -(hops[v[0]] + hops[v[1]] + hops[v[2]]) - 0.5 * v[3])
    all_peers = [along_x[x] + along_z[z] + along_y[y] + cores[c] for x, z, y, c in steps if (x, z, y, c) != (0, 0, 0, 0)]
    my_high = member * 2 + bit(6)
    my_slot = ((my_high // 8) * 4 + group_low) * 8 + my_high % 8
    cube_peers = [flipped(CUBE_BITS, k) for k in range(1, CUBE)]
    group_peers = [flipped(GROUP_BITS, k) for k in range(1, GROUPS)]
    left, right = (me + DEVICES - 1) % DEVICES, (me + 1) % DEVICES

    loads = []
    for n, (src, dst) in enumerate(
        (
            (b_h, b_v), (d_h, d_v), (agg_h, agg_v), (row_h, row_v), (cd_h, cd_v),
            (cq_h, cq_v), (ca_h, ca_v), (q_h, q_v), (a_h, a_v),
        )
    ):
        copy = pltpu.make_async_copy(src, dst, load_sem.at[n])
        copy.start()
        loads.append(copy)

    barrier = pltpu.get_barrier_semaphore()
    for peer in all_peers:
        pl.semaphore_signal(barrier, inc=1, device_id=(peer,), device_id_type=MESH)

    def send(src, dst, send_sem, recv_sem, peer):
        pltpu.make_async_remote_copy(
            src_ref=src, dst_ref=dst, send_sem=send_sem, recv_sem=recv_sem,
            device_id=(peer,), device_id_type=MESH,
        ).start()

    def wait_bytes(ref, sem):
        pltpu.make_async_copy(ref, ref, sem).wait()

    lane = lax.broadcasted_iota(I32, (1, LANES), 1)

    stage[...] = jnp.zeros_like(stage)
    pack[...] = jnp.zeros_like(pack)
    for n in range(7):
        loads[n].wait()
    w_v[...] = DAMP / d_v[...]
    s1_v[...] = w_v[...] * b_v[...]
    f1[pl.ds(0, 3), :] = s1_v[...]
    place_row = position_of(row_v[...])
    stage[pl.ds(0, 3), pl.ds(0, AGG_DEV)] = cd_v[...]
    stage[pl.ds(3, 1), pl.ds(0, AGG_DEV)] = place_row.astype(F32)
    own = stage[...]
    node_place = pick(own[3:4, :], agg_v[...])
    for n in range(BLOCKS):
        f1[pl.ds(3, 1), pl.ds(n * LANES, LANES)] = node_place[n : n + 1, :]
    line = own[0:1]
    for n in range(1, 4):
        line = jnp.where(lane // AGG_DEV == n, pltpu.roll(own, 32 * n, 1)[n : n + 1], line)
    far0[my_slot] = line
    for e in range(9):
        pack[e // 4, pl.ds(32 * (e % 4), 32), pl.ds(0, NNZ)] = ca_v[e // 3, e % 3]
    pack[2, pl.ds(32, 32), pl.ds(0, NNZ)] = position_of(cq_v[...]).astype(F32)
    for n in range(3):
        rm[group, pl.ds(32 * n, 32), :] = pack[n].T[0:32, :]

    pl.semaphore_wait(barrier, DEVICES - 1)

    def send_halo(n, own_ref, from_left, from_right):
        send(own_ref.at[:, pl.ds(NODE_DEV - WIN, WIN)], from_left, halo_send.at[n, 0], halo_recv.at[n, 0], right)
        send(own_ref.at[:, pl.ds(0, WIN)], from_right, halo_send.at[n, 1], halo_recv.at[n, 1], left)

    def wait_halo(n, from_left, from_right):
        wait_bytes(from_left, halo_recv.at[n, 0])
        wait_bytes(from_right, halo_recv.at[n, 1])

    def send_group(n, ref):
        for peer in group_peers:
            send(ref.at[group], ref.at[group], far_send.at[n], far_recv.at[n], peer)

    def send_all(n, ref):
        for peer in all_peers:
            send(ref.at[my_slot], ref.at[my_slot], far_send.at[n], far_recv.at[n], peer)

    def receive_all(n, ref, table):
        wait_bytes(ref.at[pl.ds(0, DEVICES - 1)], far_recv.at[n])
        for t in range(4):
            parts = [ref[pl.ds(32 * t + 8 * j, 8), 0, :] for j in range(4)]
            for c in range(table.shape[0]):
                whole = None
                for j in range(4):
                    moved = parts[j] if j == c else pltpu.roll(parts[j], 32 * ((j - c) % 4), 1)
                    whole = moved if j == 0 else jnp.where((lane // 32) == j, moved, whole)
                table[c, pl.ds(8 * t, 8), :] = whole

    def send_cube(ref, send_sem, recv_sem):
        for peer in cube_peers:
            send(ref.at[member], ref.at[member], send_sem, recv_sem, peer)

    send_halo(0, f1, hl1, hr1)
    send_all(0, far0)
    send_group(1, rm)

    loads[7].wait()
    q_s[pl.ds(24, 8), :] = jnp.zeros((8, NODE_DEV), I32)
    base = me * NODE_DEV - WIN
    for n in range(BLOCKS):
        cols = pl.ds(n * LANES, LANES)
        q_s[pl.ds(0, NNZ), cols] = q_v[:, cols] - (base + n * LANES)
    for n in range(BLOCKS):
        label = lax.broadcasted_iota(I32, (LANES, LANES), 0) % AGG_DEV
        onehot[:, pl.ds(n * LANES, LANES)] = (agg_v[pl.ds(n, 1), :] == label).astype(F32).astype(BF16)
    r_v[...] = jnp.zeros_like(r_v)
    loads[8].wait()

    def three(own_ref, from_left, from_right):
        def rows(c, n):
            if n < SIDE:
                return from_left[pl.ds(c, 1), pl.ds(n * LANES, LANES)]
            if n < SIDE + BLOCKS:
                return own_ref[pl.ds(c, 1), pl.ds((n - SIDE) * LANES, LANES)]
            return from_right[pl.ds(c, 1), pl.ds((n - SIDE - BLOCKS) * LANES, LANES)]

        return rows

    def couple_fine(rows):
        for n in range(BLOCKS):
            cols = pl.ds(n * LANES, LANES)
            sums = [None] * 3
            for k in range(4):
                near = gather_rows(q_s[pl.ds(8 * k, 8), cols], lambda r, c: rows(c, n + r), REACH)
                width = min(8, NNZ - 8 * k)
                for i in range(3):
                    term = None
                    for c in range(3):
                        part = a_v[i, c, pl.ds(8 * k, width), cols] * near[c][:width]
                        term = part if term is None else term + part
                    term = jnp.sum(term, axis=0, keepdims=True) if width < 8 else term
                    if k == 0:
                        sums[i] = term
                    elif width == 8:
                        sums[i] = sums[i] + term
                    else:
                        sums[i] = jnp.sum(sums[i], axis=0, keepdims=True) + term
            for i in range(3):
                y_v[pl.ds(i, 1), cols] = sums[i]

    wait_halo(0, hl1, hr1)
    couple_fine(three(f1, hl1, hr1))
    f2[...] = (1.0 + KEEP) * s1_v[...] + w_v[...] * y_v[...]
    send_halo(1, f2, hl2, hr2)

    for n in range(SIDE):
        idx_v[pl.ds(n, 1), :] = hl1[pl.ds(3, 1), pl.ds(n * LANES, LANES)].astype(I32)
        idx_v[pl.ds(SIDE + BLOCKS + n, 1), :] = hr1[pl.ds(3, 1), pl.ds(n * LANES, LANES)].astype(I32)
    for n in range(BLOCKS):
        idx_v[pl.ds(SIDE + n, 1), :] = f1[pl.ds(3, 1), pl.ds(n * LANES, LANES)].astype(I32)
    idx_v[pl.ds(12, 4), :] = jnp.zeros((4, LANES), I32)

    wait_halo(1, hl2, hr2)
    couple_fine(three(f2, hl2, hr2))
    r_v[pl.ds(0, 3), :] = b_v[...] - d_v[...] * f2[...] + y_v[...]
    rest = r_v[...]
    p0 = rest.astype(BF16).astype(F32)
    rest = rest - p0
    p1 = rest.astype(BF16).astype(F32)
    pieces = jnp.concatenate([p0, p1, rest - p1], axis=0).astype(BF16)
    sums = lax.dot_general(pieces, onehot[...], (((1,), (1,)), ((), ())), preferred_element_type=F32)
    sums = sums[0:4] + sums[8:12] + sums[16:20]
    line = sums[0:1]
    for n in range(1, 3):
        line = jnp.where(lane // AGG_DEV == n, sums[n : n + 1], line)
    far1[my_slot] = line
    send_all(2, far1)

    receive_all(0, far0, tab0)
    inverse = None
    for r in range(CROWS):
        place = tab0[3, pl.ds(r, 1), :].astype(I32)
        high, low = place >> 7, place & 127
        at_high = lax.broadcasted_iota(I32, (CROWS, LANES), 0) == high
        at_low = (lax.broadcasted_iota(I32, (LANES, LANES), 0) == low).astype(F32).astype(BF16)
        weights = jnp.concatenate(
            [
                jnp.where(at_high, jnp.float32(r), 0.0),
                jnp.where(at_high, lane.astype(F32), 0.0),
            ],
            axis=0,
        ).astype(BF16)
        term = lax.dot_general(weights, at_low, (((1,), (1,)), ((), ())), preferred_element_type=F32)
        inverse = term if inverse is None else inverse + term
    inv_v[...] = (inverse[0:CROWS] * LANES + inverse[CROWS : 2 * CROWS]).astype(I32)
    for c in range(3):
        tab0[c] = DAMP / tab0[c]
    for r in range(CROWS):
        for c in range(3):
            wbuf[r // 2, pl.ds(4 * (r % 2) + c, 1), :] = tab0[c, pl.ds(r, 1), :]
    wait_bytes(rm.at[pl.ds(0, GROUPS - 1)], far_recv.at[1])
    for h in range(2):
        for e4 in range(3):
            for k in range(4):
                parts = [rm[4 * h + j, pl.ds(32 * e4 + 8 * k, 8), :] for j in range(4)]
                for s in range(4):
                    e = 4 * e4 + s
                    if e > 9:
                        continue
                    whole = None
                    for j in range(4):
                        moved = parts[j] if j == s else pltpu.roll(parts[j], 32 * ((j - s) % 4), 1)
                        whole = moved if j == 0 else jnp.where((lane // 32) == j, moved, whole)
                    rows, cols = pl.ds(8 * k, 8), pl.ds(LANES * h, LANES)
                    if e < 9:
                        mx[e, rows, cols] = whole
                    else:
                        mp[rows, cols] = whole.astype(I32)

    receive_all(2, far1, tab1)

    for t in range(CROWS // 8):
        sums = gather_rows(inv_v[pl.ds(8 * t, 8), :], lambda r, c: tab1[c, pl.ds(r, 1), :], CROWS)
        for c in range(3):
            value = sums[c] * tab0[c, pl.ds(8 * t, 8), :]
            for n in range(8):
                r = 8 * t + n
                cbuf[0, r // 2, pl.ds(4 * (r % 2) + c, 1), :] = value[n : n + 1, :]

    unused = lax.broadcasted_iota(I32, (8, LANES), 0) % 4 == 3
    first = jnp.where(unused, 0.0, cbuf[0, member])
    weight = jnp.where(unused, 0.0, wbuf[member])

    def sweep(n, current):
        totals = []
        for h in range(2):
            cols = pl.ds(LANES * h, LANES)
            sums = [None] * 3
            for k in range(4):
                rows = pl.ds(8 * k, 8)
                near = gather_rows(mp[rows, cols], lambda r, c: cbuf[n, r // 2, pl.ds(4 * (r % 2) + c, 1), :], CROWS)
                for i in range(3):
                    for c in range(3):
                        part = mx[3 * i + c, rows, cols] * near[c]
                        sums[i] = part if sums[i] is None else sums[i] + part
            totals += [jnp.sum(s, axis=0, keepdims=True) for s in sums]
            totals.append(jnp.zeros((1, LANES), F32))
        current = KEEP * current + first + weight * jnp.concatenate(totals, axis=0)
        cbuf[n + 1, member] = current
        send_cube(cbuf.at[n + 1], sweep_send.at[n], sweep_recv.at[n])
        wait_bytes(cbuf.at[n + 1, pl.ds(0, CUBE - 1)], sweep_recv.at[n])
        return current

    last = lax.fori_loop(0, CSWEEPS - 1, sweep, first)

    for t in range(2):
        value = gather_rows(
            idx_v[pl.ds(8 * t, 8), :], lambda r, c: cbuf[CSWEEPS - 1, r // 2, pl.ds(4 * (r % 2) + c, 1), :], CROWS
        )
        rows = three(f2, hl2, hr2)
        for n in range(8 if t == 0 else 4):
            for c in range(3):
                f3[pl.ds(c, 1), pl.ds((8 * t + n) * LANES, LANES)] = rows(c, 8 * t + n) + value[c][n : n + 1, :]
    couple_fine(lambda c, n: f3[pl.ds(c, 1), pl.ds(n * LANES, LANES)])
    f4[...] = KEEP * f3[:, pl.ds(WIN, NODE_DEV)] + s1_v[...] + w_v[...] * y_v[...]
    send_halo(2, f4, hl4, hr4)

    half = jnp.where(group_high == 0, last[0:4], last[4:8])
    moved = half
    for k in range(1, 4):
        moved = jnp.where(group_low == k, pltpu.roll(half, LANES - 32 * k, 1), moved)
    cor_o[...] = moved[0:3, 0:AGG_DEV]

    wait_halo(2, hl4, hr4)
    couple_fine(three(f4, hl4, hr4))
    sol_o[...] = KEEP * f4[...] + s1_v[...] + w_v[...] * y_v[...]

    for n, from_left in enumerate((hl1, hl2, hl4)):
        wait_bytes(from_left, halo_send.at[n, 0])
        wait_bytes(from_left, halo_send.at[n, 1])
    for n, (ref, count) in enumerate(((far0, DEVICES), (rm, GROUPS), (far1, DEVICES))):
        wait_bytes(ref.at[pl.ds(0, count - 1)], far_send.at[n])
    for n in range(CSWEEPS - 1):
        wait_bytes(cbuf.at[n + 1, pl.ds(0, CUBE - 1)], sweep_send.at[n])


def body(b, d, q, a, agg, row, cd, cq, ca):
    any_spec = pl.BlockSpec(memory_space=pl.ANY)
    vmem = pl.BlockSpec(memory_space=pltpu.VMEM)
    dma = pltpu.SemaphoreType.DMA
    sol, cor = pl.pallas_call(
        kernel,
        out_shape=(
            jax.ShapeDtypeStruct((3, NODE_DEV), F32),
            jax.ShapeDtypeStruct((3, AGG_DEV), F32),
        ),
        in_specs=[any_spec] * 9,
        out_specs=(vmem, vmem),
        scratch_shapes=[
            pltpu.VMEM((3, NODE_DEV), F32),
            pltpu.VMEM((3, NODE_DEV), F32),
            pltpu.VMEM((NNZ, NODE_DEV), I32),
            pltpu.VMEM((3, 3, NNZ, NODE_DEV), F32),
            pltpu.VMEM((BLOCKS, LANES), I32),
            pltpu.VMEM((1, AGG_DEV), I32),
            pltpu.VMEM((3, AGG_DEV), F32),
            pltpu.VMEM((AGG_DEV, NNZ), I32),
            pltpu.VMEM((3, 3, AGG_DEV, NNZ), F32),
            pltpu.VMEM((3, NODE_DEV), F32),
            pltpu.VMEM((3, NODE_DEV), F32),
            pltpu.VMEM((32, NODE_DEV), I32),
            pltpu.VMEM((3, NODE_DEV), F32),
            pltpu.VMEM((8, NODE_DEV), F32),
            pltpu.VMEM((LANES, NODE_DEV), BF16),
            pltpu.VMEM((16, LANES), I32),
            pltpu.VMEM((4, NODE_DEV), F32),
            pltpu.VMEM((4, WIN), F32),
            pltpu.VMEM((4, WIN), F32),
            pltpu.VMEM((3, NODE_DEV), F32),
            pltpu.VMEM((3, WIN), F32),
            pltpu.VMEM((3, WIN), F32),
            pltpu.VMEM((3, NODE_DEV + 2 * WIN), F32),
            pltpu.VMEM((3, NODE_DEV), F32),
            pltpu.VMEM((3, WIN), F32),
            pltpu.VMEM((3, WIN), F32),
            pltpu.VMEM((4, LANES), F32),
            pltpu.VMEM((DEVICES, 1, LANES), F32),
            pltpu.VMEM((DEVICES, 1, LANES), F32),
            pltpu.VMEM((4, CROWS, LANES), F32),
            pltpu.VMEM((3, CROWS, LANES), F32),
            pltpu.VMEM((3, LANES, LANES), F32),
            pltpu.VMEM((GROUPS, 96, LANES), F32),
            pltpu.VMEM((9, 32, 2 * LANES), F32),
            pltpu.VMEM((32, 2 * LANES), I32),
            pltpu.VMEM((CROWS, LANES), I32),
            pltpu.VMEM((CUBE, 8, LANES), F32),
            pltpu.VMEM((CSWEEPS, CUBE, 8, LANES), F32),
            dma((9,)),
            dma((3, 2)),
            dma((3, 2)),
            dma((3,)),
            dma((3,)),
            dma((CSWEEPS - 1,)),
            dma((CSWEEPS - 1,)),
        ],
        compiler_params=pltpu.CompilerParams(collective_id=0, has_side_effects=True),
        name="vcycle",
    )(
        b.T,
        d.T,
        q.T,
        a.transpose(2, 3, 1, 0),
        agg.reshape(BLOCKS, LANES),
        row.reshape(1, AGG_DEV),
        cd.T,
        cq,
        ca.transpose(2, 3, 0, 1),
    )
    return sol.T, cor.T


def solution(mesh):
    rows, line = P("dom", None), P("dom")
    blocks = P("dom", None, None, None)
    return jax.shard_map(
        body,
        mesh=mesh,
        in_specs=(rows, rows, rows, blocks, line, line, rows, rows, blocks),
        out_specs=(rows, rows),
        check_vma=False,
    )
```

```python
import jax
import jax.numpy as jnp
from jax import lax
from jax.experimental import pallas as pl
from jax.experimental.pallas import tpu as pltpu
from jax.sharding import PartitionSpec as P

DEVICES = 128
NODE_DEV = 1024
WIN = 256
NNZ = 27
AGG_DEV = 32
CSWEEPS = 6
LANES = 128
BLOCKS = NODE_DEV // LANES
SIDE = WIN // LANES
WIDE = BLOCKS + 2 * SIDE
REACH = 2 * SIDE + 1
CUBE = 16
GROUPS = 8
CROWS = 32
DAMP = 0.7
KEEP = 1.0 - DAMP
CUBE_BITS = ((0,), (1,), (3,), (5,))
GROUP_BITS = ((1, 2), (3, 4), (5, 6))
MESH = pl.DeviceIdType.MESH
F32, I32, BF16 = jnp.float32, jnp.int32, jnp.bfloat16


def position_of(row):
    def bit(p):
        return (row >> p) & 1

    high = (bit(10) ^ bit(11)) * 16 + (bit(8) ^ bit(9)) * 8 + (bit(6) ^ bit(7)) * 4 + bit(5) * 2 + bit(11)
    lane = bit(9) * 64 + bit(7) * 32 + (row & 31)
    return high * LANES + lane


def spread(row):
    return jnp.broadcast_to(row, (8, LANES))


def pick(row, lane):
    return jnp.take_along_axis(spread(row), lane, axis=1, mode="promise_in_bounds")


def gather_rows(place, rows, count):
    high, lane = place >> 7, place & 127
    values = [None] * 3
    for r in range(count):
        hit = high == r
        for c in range(3):
            taken = pick(rows(r, c), lane)
            values[c] = taken if r == 0 else jnp.where(hit, taken, values[c])
    return values


def kernel(
    b_h, d_h, q_h, a_h, agg_h, row_h, cd_h, cq_h, ca_h,
    sol_o, cor_o,
    b_v, d_v, q_v, a_v, agg_v, row_v, cd_v, cq_v, ca_v,
 q_s, y_v, r_v, onehot, idx_v,
    f1, f1l, f1r, f2, f3, f4,
    stage, far0, far1, tab0, tab1,
    pack, rm, mx, mp,
    inv_v, wbuf, cbuf,
    load_sem, side_send, side_recv, entered, far_send, far_recv, sweep_send, sweep_recv,
):
    me = lax.axis_index("dom")

    def bit(p):
        return (me // (1 << p)) % 2

    member = (bit(5) + bit(6)) % 2 * 8 + (bit(3) + bit(4)) % 2 * 4 + (bit(1) + bit(2)) % 2 * 2 + bit(0)
    group = bit(6) * 4 + bit(4) * 2 + bit(2)
    group_low, group_high = bit(4) * 2 + bit(2), bit(6)

    def flipped(bits, k):
        other = me
        for n, p in enumerate(bits):
            if (k >> n) & 1:
                for q in p:
                    other = other + (1 - 2 * bit(q)) * (1 << q)
        return other

    def ring(low, high):
        at = bit(high) * 2 + bit(low)
        places = [(at + k) % 4 for k in range(4)]
        return [(v // 2) * (1 << high) + (v % 2) * (1 << low) for v in places]

    along_x, along_z, along_y = ring(1, 2), ring(3, 4), ring(5, 6)
    cores = [bit(0), 1 - bit(0)]
    steps = [(x, z, y, c) for x in range(4) for z in range(4) for y in range(4) for c in range(2)]
    hops = (0, 1, 2, 1)
    steps = sorted(steps, key=lambda v: -(hops[v[0]] + hops[v[1]] + hops[v[2]]) - 0.5 * v[3])
    all_peers = [along_x[x] + along_z[z] + along_y[y] + cores[c] for x, z, y, c in steps if (x, z, y, c) != (0, 0, 0, 0)]
    my_high = member * 2 + bit(6)
    my_slot = ((my_high // 8) * 4 + group_low) * 8 + my_high % 8
    cube_peers = [flipped(CUBE_BITS, k) for k in range(1, CUBE)]
    group_peers = [flipped(GROUP_BITS, k) for k in range(1, GROUPS)]
    left, right = (me + DEVICES - 1) % DEVICES, (me + 1) % DEVICES

    loads = []
    for n, (src, dst) in enumerate(
        (
            (b_h, b_v), (d_h, d_v), (agg_h, agg_v), (row_h, row_v), (cd_h, cd_v),
            (cq_h, cq_v), (ca_h, ca_v), (q_h, q_v), (a_h, a_v),
        )
    ):
        copy = pltpu.make_async_copy(src, dst, load_sem.at[n])
        copy.start()
        loads.append(copy)

    barrier = pltpu.get_barrier_semaphore()
    for peer in cube_peers + group_peers + [left, right]:
        pl.semaphore_signal(barrier, inc=1, device_id=(peer,), device_id_type=MESH)

    def send(src, dst, send_sem, recv_sem, peer):
        pltpu.make_async_remote_copy(
            src_ref=src, dst_ref=dst, send_sem=send_sem, recv_sem=recv_sem,
            device_id=(peer,), device_id_type=MESH,
        ).start()

    def wait_bytes(ref, sem):
        pltpu.make_async_copy(ref, ref, sem).wait()

    lane = lax.broadcasted_iota(I32, (1, LANES), 1)

    def cols(n, count=1):
        return pl.ds(n * LANES, count * LANES)

    for n in range(4):
        loads[n].wait()
    place_row = position_of(row_v[...])
    stage[...] = jnp.zeros_like(stage)
    stage[pl.ds(3, 1), pl.ds(0, AGG_DEV)] = place_row.astype(F32)
    node_place = pick(stage[pl.ds(3, 1), :], agg_v[...])
    w0 = DAMP / d_v[...]
    f1[pl.ds(0, 3), :] = w0 * b_v[...]
    f1[pl.ds(4, 3), :] = w0
    for n in range(BLOCKS):
        f1[pl.ds(3, 1), cols(n)] = node_place[n : n + 1, :]
    for n in range(4, 9):
        loads[n].wait()
    pl.semaphore_wait(barrier, CUBE - 1 + GROUPS - 1 + 2)

    def to_right(n, src, dst):
        return pltpu.make_async_remote_copy(
            src_ref=src, dst_ref=dst, send_sem=side_send.at[n, 0], recv_sem=side_recv.at[n, 0],
            device_id=(right,), device_id_type=MESH,
        )

    def to_left(n, src, dst):
        return pltpu.make_async_remote_copy(
            src_ref=src, dst_ref=dst, send_sem=side_send.at[n, 1], recv_sem=side_recv.at[n, 1],
            device_id=(left,), device_id_type=MESH,
        )

    own_end, own_start = pl.ds(NODE_DEV, WIN), pl.ds(WIN, WIN)
    from_left, from_right = pl.ds(0, WIN), pl.ds(NODE_DEV + WIN, WIN)
    rightward = [
        to_right(0, f1.at[:, pl.ds(NODE_DEV - WIN, WIN)], f1l),
        to_right(1, f2.at[:, own_end], f2.at[:, from_left]),
        to_right(2, f4.at[:, own_end], f4.at[:, from_left]),
    ]
    leftward = [
        to_left(0, f1.at[:, pl.ds(0, WIN)], f1r),
        to_left(1, f2.at[:, own_start], f2.at[:, from_right]),
        to_left(2, f4.at[:, own_start], f4.at[:, from_right]),
    ]
    has_left, has_right = me > 0, me < DEVICES - 1

    def start_sides(n):
        pl.when(has_right)(rightward[n].start)
        pl.when(has_left)(leftward[n].start)

    def await_sides(n):
        pl.when(has_left)(rightward[n].wait_recv)
        pl.when(has_right)(leftward[n].wait_recv)

    start_sides(0)
    for peer in group_peers:
        pl.semaphore_signal(entered, inc=1, device_id=(peer,), device_id_type=MESH)

    stage[pl.ds(0, 3), pl.ds(0, AGG_DEV)] = cd_v[...]
    own = stage[...]
    line = own[0:1]
    for n in range(1, 4):
        line = jnp.where(lane // AGG_DEV == n, pltpu.roll(own, 32 * n, 1)[n : n + 1], line)
    far0[my_slot] = line

    def send_group(n, ref):
        for peer in group_peers:
            send(ref.at[group], ref.at[group], far_send.at[n], far_recv.at[n], peer)

    def send_all(n, ref):
        for peer in all_peers:
            send(ref.at[my_slot], ref.at[my_slot], far_send.at[n], far_recv.at[n], peer)

    def receive_all(n, ref, table):
        wait_bytes(ref.at[pl.ds(0, DEVICES - 1)], far_recv.at[n])
        for t in range(4):
            parts = [ref[pl.ds(32 * t + 8 * j, 8), 0, :] for j in range(4)]
            for c in range(table.shape[0]):
                whole = None
                for j in range(4):
                    moved = parts[j] if j == c else pltpu.roll(parts[j], 32 * ((j - c) % 4), 1)
                    whole = moved if j == 0 else jnp.where((lane // 32) == j, moved, whole)
                table[c, pl.ds(8 * t, 8), :] = whole

    def send_cube(ref, send_sem, recv_sem):
        for peer in cube_peers:
            send(ref.at[member], ref.at[member], send_sem, recv_sem, peer)

    def number_columns(n, carry):
        here = pl.ds(pl.multiple_of(n * LANES, LANES), LANES)
        q_s[pl.ds(24, 8), here] = jnp.zeros((8, LANES), I32)
        q_s[pl.ds(0, NNZ), here] = q_v[:, here] - (me * NODE_DEV - WIN + n * LANES)
        return carry

    def pack_one(e, carry):
        pack[e // 4, pl.ds(pl.multiple_of(32 * (e % 4), 32), 32), pl.ds(0, NNZ)] = ca_v[e // 3, e % 3]
        return carry

    pack[...] = jnp.zeros_like(pack)
    lax.fori_loop(0, 9, pack_one, 0)
    pack[2, pl.ds(32, 32), pl.ds(0, NNZ)] = position_of(cq_v[...]).astype(F32)
    for n in range(3):
        rm[group, pl.ds(32 * n, 32), :] = pack[n].T[0:32, :]
    send_group(1, rm)

    lax.fori_loop(0, BLOCKS, number_columns, 0)

    def couple_fine(blocks, field):
        for n in blocks:
            here = cols(n - SIDE)
            sums = [None] * 3
            for k in range(4):
                near = gather_rows(q_s[pl.ds(8 * k, 8), here], lambda r, c: field(c, n + r - SIDE), REACH)
                width = min(8, NNZ - 8 * k)
                for i in range(3):
                    term = None
                    for c in range(3):
                        part = a_v[i, c, pl.ds(8 * k, width), here] * near[c][:width]
                        term = part if term is None else term + part
                    term = jnp.sum(term, axis=0, keepdims=True) if width < 8 else term
                    if k == 0:
                        sums[i] = term
                    elif width == 8:
                        sums[i] = sums[i] + term
                    else:
                        sums[i] = jnp.sum(sums[i], axis=0, keepdims=True) + term
            for i in range(3):
                y_v[pl.ds(i, 1), here] = sums[i]

    def first_field(row, n, count=1):
        if n < SIDE:
            return f1l[row, cols(n, count)]
        if n < SIDE + BLOCKS:
            return f1[row, cols(n - SIDE, count)]
        return f1r[row, cols(n - SIDE - BLOCKS, count)]

    def start_field(c, n):
        return first_field(pl.ds(c, 1), n)

    middle = range(2 * SIDE, BLOCKS)
    border = [*range(SIDE, 2 * SIDE), *range(BLOCKS, BLOCKS + SIDE)]
    values, weights_at = pl.ds(0, 3), pl.ds(4, 3)

    couple_fine(middle, start_field)
    pl.semaphore_wait(entered, GROUPS - 1)
    send_all(0, far0)

    await_sides(0)
    couple_fine(border, start_field)
    inside = cols(SIDE, BLOCKS)
    f2[:, inside] = (1.0 + KEEP) * f1[values, :] + f1[weights_at, :] * y_v[...]
    start_sides(1)
    couple_fine(middle, lambda c, n: f2[pl.ds(c, 1), cols(n)])

    def label_block(n, carry):
        label = lax.broadcasted_iota(I32, (LANES, LANES), 0) % AGG_DEV
        hit = agg_v[pl.ds(n, 1), :] == label
        onehot[:, pl.ds(pl.multiple_of(n * LANES, LANES), LANES)] = hit.astype(F32).astype(BF16)
        return carry

    lax.fori_loop(0, BLOCKS, label_block, 0)
    r_v[...] = jnp.zeros_like(r_v)
    await_sides(1)
    couple_fine(border, lambda c, n: f2[pl.ds(c, 1), cols(n)])
    r_v[pl.ds(0, 3), :] = b_v[...] - d_v[...] * f2[:, inside] + y_v[...]
    rest = r_v[...]
    p0 = rest.astype(BF16).astype(F32)
    rest = rest - p0
    p1 = rest.astype(BF16).astype(F32)
    pieces = jnp.concatenate([p0, p1, rest - p1], axis=0).astype(BF16)
    sums = lax.dot_general(pieces, onehot[...], (((1,), (1,)), ((), ())), preferred_element_type=F32)
    sums = sums[0:4] + sums[8:12] + sums[16:20]
    line = sums[0:1]
    for n in range(1, 3):
        line = jnp.where(lane // AGG_DEV == n, sums[n : n + 1], line)
    far1[my_slot] = line
    send_all(2, far1)

    receive_all(0, far0, tab0)
    inverse = None
    for r in range(CROWS):
        place = tab0[3, pl.ds(r, 1), :].astype(I32)
        high, low = place >> 7, place & 127
        at_high = lax.broadcasted_iota(I32, (CROWS, LANES), 0) == high
        at_low = (lax.broadcasted_iota(I32, (LANES, LANES), 0) == low).astype(F32).astype(BF16)
        weights = jnp.concatenate(
            [
                jnp.where(at_high, jnp.float32(r), 0.0),
                jnp.where(at_high, lane.astype(F32), 0.0),
            ],
            axis=0,
        ).astype(BF16)
        term = lax.dot_general(weights, at_low, (((1,), (1,)), ((), ())), preferred_element_type=F32)
        inverse = term if inverse is None else inverse + term
    inv_v[...] = (inverse[0:CROWS] * LANES + inverse[CROWS : 2 * CROWS]).astype(I32)
    for c in range(3):
        tab0[c] = DAMP / tab0[c]
    for r in range(CROWS):
        for c in range(3):
            wbuf[r // 2, pl.ds(4 * (r % 2) + c, 1), :] = tab0[c, pl.ds(r, 1), :]
    wait_bytes(rm.at[pl.ds(0, GROUPS - 1)], far_recv.at[1])
    for h in range(2):
        for e4 in range(3):
            for k in range(4):
                parts = [rm[4 * h + j, pl.ds(32 * e4 + 8 * k, 8), :] for j in range(4)]
                for s in range(4):
                    e = 4 * e4 + s
                    if e > 9:
                        continue
                    whole = None
                    for j in range(4):
                        moved = parts[j] if j == s else pltpu.roll(parts[j], 32 * ((j - s) % 4), 1)
                        whole = moved if j == 0 else jnp.where((lane // 32) == j, moved, whole)
                    rows, lines = pl.ds(8 * k, 8), pl.ds(LANES * h, LANES)
                    if e < 9:
                        mx[e, rows, lines] = whole
                    else:
                        mp[rows, lines] = whole.astype(I32)

    idx_v[...] = jnp.zeros_like(idx_v)
    for n in range(WIDE):
        idx_v[pl.ds(n, 1), :] = first_field(pl.ds(3, 1), n).astype(I32)

    receive_all(2, far1, tab1)

    for t in range(CROWS // 8):
        sums = gather_rows(inv_v[pl.ds(8 * t, 8), :], lambda r, c: tab1[c, pl.ds(r, 1), :], CROWS)
        for c in range(3):
            value = sums[c] * tab0[c, pl.ds(8 * t, 8), :]
            for n in range(8):
                r = 8 * t + n
                cbuf[0, r // 2, pl.ds(4 * (r % 2) + c, 1), :] = value[n : n + 1, :]

    unused = lax.broadcasted_iota(I32, (8, LANES), 0) % 4 == 3
    first = jnp.where(unused, 0.0, cbuf[0, member])
    weight = jnp.where(unused, 0.0, wbuf[member])

    def sweep(n, current):
        totals = []
        for h in range(2):
            lines = pl.ds(LANES * h, LANES)
            sums = [None] * 3
            for k in range(4):
                rows = pl.ds(8 * k, 8)
                near = gather_rows(mp[rows, lines], lambda r, c: cbuf[n, r // 2, pl.ds(4 * (r % 2) + c, 1), :], CROWS)
                for i in range(3):
                    for c in range(3):
                        part = mx[3 * i + c, rows, lines] * near[c]
                        sums[i] = part if sums[i] is None else sums[i] + part
            totals += [jnp.sum(s, axis=0, keepdims=True) for s in sums]
            totals.append(jnp.zeros((1, LANES), F32))
        current = KEEP * current + first + weight * jnp.concatenate(totals, axis=0)
        cbuf[n + 1, member] = current
        send_cube(cbuf.at[n + 1], sweep_send.at[n], sweep_recv.at[n])
        wait_bytes(cbuf.at[n + 1, pl.ds(0, CUBE - 1)], sweep_recv.at[n])
        return current

    last = lax.fori_loop(0, CSWEEPS - 1, sweep, first)

    for t in range(2):
        value = gather_rows(
            idx_v[pl.ds(8 * t, 8), :], lambda r, c: cbuf[CSWEEPS - 1, r // 2, pl.ds(4 * (r % 2) + c, 1), :], CROWS
        )
        for n in range(8 * t, min(8 * t + 8, WIDE)):
            for c in range(3):
                f3[pl.ds(c, 1), cols(n)] = f2[pl.ds(c, 1), cols(n)] + value[c][n - 8 * t : n - 8 * t + 1, :]

    def smooth(old, n, count):
        here = cols(n - SIDE, count)
        return KEEP * old[:, cols(n, count)] + f1[values, here] + f1[weights_at, here] * y_v[:, here]

    couple_fine(border, lambda c, n: f3[pl.ds(c, 1), cols(n)])
    for n in (SIDE, BLOCKS):
        f4[:, cols(n, SIDE)] = smooth(f3, n, SIDE)
    start_sides(2)
    couple_fine(middle, lambda c, n: f3[pl.ds(c, 1), cols(n)])
    f4[:, cols(2 * SIDE, BLOCKS - 2 * SIDE)] = smooth(f3, 2 * SIDE, BLOCKS - 2 * SIDE)
    couple_fine(middle, lambda c, n: f4[pl.ds(c, 1), cols(n)])

    part = jnp.where(group_high == 0, last[0:4], last[4:8])
    moved = part
    for k in range(1, 4):
        moved = jnp.where(group_low == k, pltpu.roll(part, LANES - 32 * k, 1), moved)
    cor_o[...] = moved[0:3, 0:AGG_DEV]

    await_sides(2)
    couple_fine(border, lambda c, n: f4[pl.ds(c, 1), cols(n)])
    sol_o[...] = smooth(f4, SIDE, BLOCKS)

    for n in range(3):
        pl.when(has_right)(rightward[n].wait_send)
        pl.when(has_left)(leftward[n].wait_send)
    for n, (ref, count) in enumerate(((far0, DEVICES), (rm, GROUPS), (far1, DEVICES))):
        wait_bytes(ref.at[pl.ds(0, count - 1)], far_send.at[n])
    for n in range(CSWEEPS - 1):
        wait_bytes(cbuf.at[n + 1, pl.ds(0, CUBE - 1)], sweep_send.at[n])


def body(b, d, q, a, agg, row, cd, cq, ca):
    any_spec = pl.BlockSpec(memory_space=pl.ANY)
    vmem = pl.BlockSpec(memory_space=pltpu.VMEM)
    dma = pltpu.SemaphoreType.DMA
    sol, cor = pl.pallas_call(
        kernel,
        out_shape=(
            jax.ShapeDtypeStruct((3, NODE_DEV), F32),
            jax.ShapeDtypeStruct((3, AGG_DEV), F32),
        ),
        in_specs=[any_spec] * 9,
        out_specs=(vmem, vmem),
        scratch_shapes=[
            pltpu.VMEM((3, NODE_DEV), F32),
            pltpu.VMEM((3, NODE_DEV), F32),
            pltpu.VMEM((NNZ, NODE_DEV), I32),
            pltpu.VMEM((3, 3, NNZ, NODE_DEV), F32),
            pltpu.VMEM((BLOCKS, LANES), I32),
            pltpu.VMEM((1, AGG_DEV), I32),
            pltpu.VMEM((3, AGG_DEV), F32),
            pltpu.VMEM((AGG_DEV, NNZ), I32),
            pltpu.VMEM((3, 3, AGG_DEV, NNZ), F32),
            pltpu.VMEM((32, NODE_DEV), I32),
            pltpu.VMEM((3, NODE_DEV), F32),
            pltpu.VMEM((8, NODE_DEV), F32),
            pltpu.VMEM((LANES, NODE_DEV), BF16),
            pltpu.VMEM((16, LANES), I32),
            pltpu.VMEM((8, NODE_DEV), F32),
            pltpu.VMEM((8, WIN), F32),
            pltpu.VMEM((8, WIN), F32),
            pltpu.VMEM((3, WIDE * LANES), F32),
            pltpu.VMEM((3, WIDE * LANES), F32),
            pltpu.VMEM((3, WIDE * LANES), F32),
            pltpu.VMEM((4, LANES), F32),
            pltpu.VMEM((DEVICES, 1, LANES), F32),
            pltpu.VMEM((DEVICES, 1, LANES), F32),
            pltpu.VMEM((4, CROWS, LANES), F32),
            pltpu.VMEM((3, CROWS, LANES), F32),
            pltpu.VMEM((3, LANES, LANES), F32),
            pltpu.VMEM((GROUPS, 96, LANES), F32),
            pltpu.VMEM((9, 32, 2 * LANES), F32),
            pltpu.VMEM((32, 2 * LANES), I32),
            pltpu.VMEM((CROWS, LANES), I32),
            pltpu.VMEM((CUBE, 8, LANES), F32),
            pltpu.VMEM((CSWEEPS, CUBE, 8, LANES), F32),
            dma((9,)),
            dma((3, 2)),
            dma((3, 2)),
            pltpu.SemaphoreType.REGULAR,
            dma((3,)),
            dma((3,)),
            dma((CSWEEPS - 1,)),
            dma((CSWEEPS - 1,)),
        ],
        compiler_params=pltpu.CompilerParams(collective_id=0, has_side_effects=True),
        name="vcycle",
    )(
        b.T,
        d.T,
        q.T,
        a.transpose(2, 3, 1, 0),
        agg.reshape(BLOCKS, LANES),
        row.reshape(1, AGG_DEV),
        cd.T,
        cq,
        ca.transpose(2, 3, 0, 1),
    )
    return sol.T, cor.T


def solution(mesh):
    rows, line = P("dom", None), P("dom")
    blocks = P("dom", None, None, None)
    return jax.shard_map(
        body,
        mesh=mesh,
        in_specs=(rows, rows, rows, blocks, line, line, rows, rows, blocks),
        out_specs=(rows, rows),
        check_vma=False,
    )
```

```python
import jax
import jax.numpy as jnp
from jax import lax
from jax.experimental import pallas as pl
from jax.experimental.pallas import tpu as pltpu
from jax.sharding import PartitionSpec as P

DEVICES = 128
NODE_DEV = 1024
WIN = 256
NNZ = 27
AGG_DEV = 32
CSWEEPS = 6
LANES = 128
BLOCKS = NODE_DEV // LANES
SIDE = WIN // LANES
WIDE = BLOCKS + 2 * SIDE
REACH = 2 * SIDE + 1
CUBE = 16
GROUPS = 8
CROWS = 32
DAMP = 0.7
KEEP = 1.0 - DAMP
CUBE_BITS = ((0,), (1,), (3,), (5,))
GROUP_BITS = ((1, 2), (3, 4), (5, 6))
MESH = pl.DeviceIdType.MESH
F32, I32, BF16 = jnp.float32, jnp.int32, jnp.bfloat16


def position_of(row):
    def bit(p):
        return (row >> p) & 1

    high = (bit(10) ^ bit(11)) * 16 + (bit(8) ^ bit(9)) * 8 + (bit(6) ^ bit(7)) * 4 + bit(5) * 2 + bit(11)
    lane = bit(9) * 64 + bit(7) * 32 + (row & 31)
    return high * LANES + lane


def spread(row):
    return jnp.broadcast_to(row, (8, LANES))


def pick(row, lane):
    return jnp.take_along_axis(spread(row), lane, axis=1, mode="promise_in_bounds")


def gather_rows(place, rows, count):
    high, lane = place >> 7, place & 127
    values = [None] * 3
    for r in range(count):
        hit = high == r
        for c in range(3):
            taken = pick(rows(r, c), lane)
            values[c] = taken if r == 0 else jnp.where(hit, taken, values[c])
    return values


def kernel(
    b_h, d_h, q_h, a_h, agg_h, row_h, cd_h, cq_h, ca_h,
    sol_o, cor_o,
    b_v, d_v, q_v, a_v, agg_v, row_v, cd_v, cq_v, ca_v,
 q_s, y_v, r_v, onehot, idx_v,
    f1, f1l, f1r, f2, f3, f4,
    stage, far0, far1, tab0, tab1,
    pack, rm, mx, mp,
    inv_v, wbuf, cbuf,
    load_sem, side_send, side_recv, entered, far_send, far_recv, sweep_send, sweep_recv,
):
    me = lax.axis_index("dom")

    def bit(p):
        return (me // (1 << p)) % 2

    member = (bit(5) + bit(6)) % 2 * 8 + (bit(3) + bit(4)) % 2 * 4 + (bit(1) + bit(2)) % 2 * 2 + bit(0)
    group = bit(6) * 4 + bit(4) * 2 + bit(2)
    group_low, group_high = bit(4) * 2 + bit(2), bit(6)

    def flipped(bits, k):
        other = me
        for n, p in enumerate(bits):
            if (k >> n) & 1:
                for q in p:
                    other = other + (1 - 2 * bit(q)) * (1 << q)
        return other

    def ring(low, high):
        at = bit(high) * 2 + bit(low)
        places = [(at + k) % 4 for k in range(4)]
        return [(v // 2) * (1 << high) + (v % 2) * (1 << low) for v in places]

    along_x, along_z, along_y = ring(1, 2), ring(3, 4), ring(5, 6)
    cores = [bit(0), 1 - bit(0)]
    steps = [(x, z, y, c) for x in range(4) for z in range(4) for y in range(4) for c in range(2)]
    hops = (0, 1, 2, 1)
    steps = sorted(steps, key=lambda v: -(hops[v[0]] + hops[v[1]] + hops[v[2]]) - 0.5 * v[3])
    all_peers = [along_x[x] + along_z[z] + along_y[y] + cores[c] for x, z, y, c in steps if (x, z, y, c) != (0, 0, 0, 0)]
    my_high = member * 2 + bit(6)
    my_slot = ((my_high // 8) * 4 + group_low) * 8 + my_high % 8
    cube_peers = [flipped(CUBE_BITS, k) for k in range(1, CUBE)]
    group_peers = [flipped(GROUP_BITS, k) for k in range(1, GROUPS)]
    left, right = (me + DEVICES - 1) % DEVICES, (me + 1) % DEVICES

    loads = []
    for n, (src, dst) in enumerate(
        (
            (b_h, b_v), (d_h, d_v), (agg_h, agg_v), (row_h, row_v), (cd_h, cd_v),
            (cq_h, cq_v), (ca_h, ca_v), (q_h, q_v), (a_h, a_v),
        )
    ):
        copy = pltpu.make_async_copy(src, dst, load_sem.at[n])
        copy.start()
        loads.append(copy)

    barrier = pltpu.get_barrier_semaphore()
    for peer in cube_peers + group_peers + [left, right]:
        pl.semaphore_signal(barrier, inc=1, device_id=(peer,), device_id_type=MESH)

    def send(src, dst, send_sem, recv_sem, peer):
        pltpu.make_async_remote_copy(
            src_ref=src, dst_ref=dst, send_sem=send_sem, recv_sem=recv_sem,
            device_id=(peer,), device_id_type=MESH,
        ).start()

    def wait_bytes(ref, sem):
        pltpu.make_async_copy(ref, ref, sem).wait()

    lane = lax.broadcasted_iota(I32, (1, LANES), 1)

    def cols(n, count=1):
        return pl.ds(n * LANES, count * LANES)

    for n in range(4):
        loads[n].wait()
    place_row = position_of(row_v[...])
    stage[...] = jnp.zeros_like(stage)
    stage[pl.ds(3, 1), pl.ds(0, AGG_DEV)] = place_row.astype(F32)
    node_place = pick(stage[pl.ds(3, 1), :], agg_v[...])
    w0 = DAMP / d_v[...]
    f1[pl.ds(0, 3), :] = w0 * b_v[...]
    f1[pl.ds(4, 3), :] = w0
    for n in range(BLOCKS):
        f1[pl.ds(3, 1), cols(n)] = node_place[n : n + 1, :]
    pl.semaphore_wait(barrier, CUBE - 1 + GROUPS - 1 + 2)

    def to_right(n, src, dst):
        return pltpu.make_async_remote_copy(
            src_ref=src, dst_ref=dst, send_sem=side_send.at[n, 0], recv_sem=side_recv.at[n, 0],
            device_id=(right,), device_id_type=MESH,
        )

    def to_left(n, src, dst):
        return pltpu.make_async_remote_copy(
            src_ref=src, dst_ref=dst, send_sem=side_send.at[n, 1], recv_sem=side_recv.at[n, 1],
            device_id=(left,), device_id_type=MESH,
        )

    own_end, own_start = pl.ds(NODE_DEV, WIN), pl.ds(WIN, WIN)
    from_left, from_right = pl.ds(0, WIN), pl.ds(NODE_DEV + WIN, WIN)
    rightward = [
        to_right(0, f1.at[:, pl.ds(NODE_DEV - WIN, WIN)], f1l),
        to_right(1, f2.at[:, own_end], f2.at[:, from_left]),
        to_right(2, f4.at[:, own_end], f4.at[:, from_left]),
    ]
    leftward = [
        to_left(0, f1.at[:, pl.ds(0, WIN)], f1r),
        to_left(1, f2.at[:, own_start], f2.at[:, from_right]),
        to_left(2, f4.at[:, own_start], f4.at[:, from_right]),
    ]
    has_left, has_right = me > 0, me < DEVICES - 1

    def start_sides(n):
        pl.when(has_right)(rightward[n].start)
        pl.when(has_left)(leftward[n].start)

    def await_sides(n):
        pl.when(has_left)(rightward[n].wait_recv)
        pl.when(has_right)(leftward[n].wait_recv)

    start_sides(0)
    for peer in group_peers:
        pl.semaphore_signal(entered, inc=1, device_id=(peer,), device_id_type=MESH)

    for n in range(4, 9):
        loads[n].wait()
    stage[pl.ds(0, 3), pl.ds(0, AGG_DEV)] = cd_v[...]
    own = stage[...]
    line = own[0:1]
    for n in range(1, 4):
        line = jnp.where(lane // AGG_DEV == n, pltpu.roll(own, 32 * n, 1)[n : n + 1], line)
    far0[my_slot] = line

    def send_group(n, ref):
        for peer in group_peers:
            send(ref.at[group], ref.at[group], far_send.at[n], far_recv.at[n], peer)

    def send_all(n, ref):
        for peer in all_peers:
            send(ref.at[my_slot], ref.at[my_slot], far_send.at[n], far_recv.at[n], peer)

    def receive_all(n, ref, table):
        wait_bytes(ref.at[pl.ds(0, DEVICES - 1)], far_recv.at[n])
        for t in range(4):
            parts = [ref[pl.ds(32 * t + 8 * j, 8), 0, :] for j in range(4)]
            for c in range(table.shape[0]):
                whole = None
                for j in range(4):
                    moved = parts[j] if j == c else pltpu.roll(parts[j], 32 * ((j - c) % 4), 1)
                    whole = moved if j == 0 else jnp.where((lane // 32) == j, moved, whole)
                table[c, pl.ds(8 * t, 8), :] = whole

    def number_columns(n, carry):
        here = pl.ds(pl.multiple_of(n * LANES, LANES), LANES)
        q_s[pl.ds(24, 8), here] = jnp.zeros((8, LANES), I32)
        q_s[pl.ds(0, NNZ), here] = q_v[:, here] - (me * NODE_DEV - WIN + n * LANES)
        return carry

    def pack_one(e, carry):
        pack[e // 4, pl.ds(pl.multiple_of(32 * (e % 4), 32), 32), pl.ds(0, NNZ)] = ca_v[e // 3, e % 3]
        return carry

    pack[...] = jnp.zeros_like(pack)
    lax.fori_loop(0, 9, pack_one, 0)
    pack[2, pl.ds(32, 32), pl.ds(0, NNZ)] = position_of(cq_v[...]).astype(F32)
    for n in range(3):
        rm[group, pl.ds(32 * n, 32), :] = pack[n].T[0:32, :]

    lax.fori_loop(0, BLOCKS, number_columns, 0)

    def label_block(n, carry):
        label = lax.broadcasted_iota(I32, (LANES, LANES), 0) % AGG_DEV
        hit = agg_v[pl.ds(n, 1), :] == label
        onehot[:, pl.ds(pl.multiple_of(n * LANES, LANES), LANES)] = hit.astype(F32).astype(BF16)
        return carry

    lax.fori_loop(0, BLOCKS, label_block, 0)

    def couple_fine(blocks, field):
        for n in blocks:
            here = cols(n - SIDE)
            sums = [None] * 3
            for k in range(4):
                near = gather_rows(q_s[pl.ds(8 * k, 8), here], lambda r, c: field(c, n + r - SIDE), REACH)
                width = min(8, NNZ - 8 * k)
                for i in range(3):
                    term = None
                    for c in range(3):
                        part = a_v[i, c, pl.ds(8 * k, width), here] * near[c][:width]
                        term = part if term is None else term + part
                    term = jnp.sum(term, axis=0, keepdims=True) if width < 8 else term
                    if k == 0:
                        sums[i] = term
                    elif width == 8:
                        sums[i] = sums[i] + term
                    else:
                        sums[i] = jnp.sum(sums[i], axis=0, keepdims=True) + term
            for i in range(3):
                y_v[pl.ds(i, 1), here] = sums[i]

    def first_field(row, n, count=1):
        if n < SIDE:
            return f1l[row, cols(n, count)]
        if n < SIDE + BLOCKS:
            return f1[row, cols(n - SIDE, count)]
        return f1r[row, cols(n - SIDE - BLOCKS, count)]

    def start_field(c, n):
        return first_field(pl.ds(c, 1), n)

    middle = range(2 * SIDE, BLOCKS)
    border = [*range(SIDE, 2 * SIDE), *range(BLOCKS, BLOCKS + SIDE)]
    values, weights_at = pl.ds(0, 3), pl.ds(4, 3)

    couple_fine(middle, start_field)

    await_sides(0)
    couple_fine(border, start_field)
    inside = cols(SIDE, BLOCKS)
    f2[:, inside] = (1.0 + KEEP) * f1[values, :] + f1[weights_at, :] * y_v[...]
    start_sides(1)
    pl.semaphore_wait(entered, GROUPS - 1)
    send_all(0, far0)
    send_group(1, rm)
    couple_fine(middle, lambda c, n: f2[pl.ds(c, 1), cols(n)])

    r_v[...] = jnp.zeros_like(r_v)
    await_sides(1)
    couple_fine(border, lambda c, n: f2[pl.ds(c, 1), cols(n)])
    r_v[pl.ds(0, 3), :] = b_v[...] - d_v[...] * f2[:, inside] + y_v[...]
    rest = r_v[...]
    p0 = rest.astype(BF16).astype(F32)
    rest = rest - p0
    p1 = rest.astype(BF16).astype(F32)
    pieces = jnp.concatenate([p0, p1, rest - p1], axis=0).astype(BF16)
    sums = lax.dot_general(pieces, onehot[...], (((1,), (1,)), ((), ())), preferred_element_type=F32)
    sums = sums[0:4] + sums[8:12] + sums[16:20]
    line = sums[0:1]
    for n in range(1, 3):
        line = jnp.where(lane // AGG_DEV == n, sums[n : n + 1], line)
    far1[my_slot] = line
    send_all(2, far1)

    receive_all(0, far0, tab0)
    inverse = None
    for r in range(CROWS):
        place = tab0[3, pl.ds(r, 1), :].astype(I32)
        high, low = place >> 7, place & 127
        at_high = lax.broadcasted_iota(I32, (CROWS, LANES), 0) == high
        at_low = (lax.broadcasted_iota(I32, (LANES, LANES), 0) == low).astype(F32).astype(BF16)
        weights = jnp.concatenate(
            [
                jnp.where(at_high, jnp.float32(r), 0.0),
                jnp.where(at_high, lane.astype(F32), 0.0),
            ],
            axis=0,
        ).astype(BF16)
        term = lax.dot_general(weights, at_low, (((1,), (1,)), ((), ())), preferred_element_type=F32)
        inverse = term if inverse is None else inverse + term
    inv_v[...] = (inverse[0:CROWS] * LANES + inverse[CROWS : 2 * CROWS]).astype(I32)
    for c in range(3):
        tab0[c] = DAMP / tab0[c]
    for r in range(CROWS):
        for c in range(3):
            wbuf[r // 2, pl.ds(4 * (r % 2) + c, 1), :] = tab0[c, pl.ds(r, 1), :]
    wait_bytes(rm.at[pl.ds(0, GROUPS - 1)], far_recv.at[1])
    for h in range(2):
        for e4 in range(3):
            for k in range(4):
                parts = [rm[4 * h + j, pl.ds(32 * e4 + 8 * k, 8), :] for j in range(4)]
                for s in range(4):
                    e = 4 * e4 + s
                    if e > 9:
                        continue
                    whole = None
                    for j in range(4):
                        moved = parts[j] if j == s else pltpu.roll(parts[j], 32 * ((j - s) % 4), 1)
                        whole = moved if j == 0 else jnp.where((lane // 32) == j, moved, whole)
                    rows, lines = pl.ds(8 * k, 8), pl.ds(LANES * h, LANES)
                    if e < 9:
                        mx[e, rows, lines] = whole
                    else:
                        mp[rows, lines] = whole.astype(I32)

    idx_v[...] = jnp.zeros_like(idx_v)
    for n in range(WIDE):
        idx_v[pl.ds(n, 1), :] = first_field(pl.ds(3, 1), n).astype(I32)

    receive_all(2, far1, tab1)

    for t in range(CROWS // 8):
        sums = gather_rows(inv_v[pl.ds(8 * t, 8), :], lambda r, c: tab1[c, pl.ds(r, 1), :], CROWS)
        for c in range(3):
            value = sums[c] * tab0[c, pl.ds(8 * t, 8), :]
            for n in range(8):
                r = 8 * t + n
                cbuf[0, r // 2, pl.ds(4 * (r % 2) + c, 1), :] = value[n : n + 1, :]

    unused = lax.broadcasted_iota(I32, (8, LANES), 0) % 4 == 3
    first = jnp.where(unused, 0.0, cbuf[0, member])
    weight = jnp.where(unused, 0.0, wbuf[member])

    def place(k):
        slot = member
        for p, w in enumerate((1, 2, 4, 8)):
            if (k >> p) & 1:
                slot = slot + (1 - 2 * ((member // w) % 2)) * w
        return slot

    stages = [[k for k in range(CUBE) if bin(k >> 1).count("1") == hops] for hops in range(4)]

    def coarse_values(n, places, arrive):
        found = [[jnp.zeros((8, LANES), F32)] * 3 for _ in places]
        for stage_of in stages:
            for k in stage_of:
                if k and arrive:
                    there = cbuf.at[n, place(k)]
                    pltpu.make_async_copy(there, there, sweep_recv.at[n - 1, k]).wait()
            for t, where in enumerate(places):
                high, low = where() >> 7, where() & 127
                for k in stage_of:
                    slot = place(k)
                    for h in range(2):
                        hit = high == slot * 2 + h
                        for c in range(3):
                            taken = pick(cbuf[n, slot, pl.ds(4 * h + c, 1), :], low)
                            found[t][c] = jnp.where(hit, taken, found[t][c])
        return found

    tiles = [(pl.ds(8 * k, 8), pl.ds(LANES * h, LANES)) for h in range(2) for k in range(4)]

    def sweep(n, current, arrive):
        near = coarse_values(n, [lambda at=at: mp[at] for at in tiles], arrive)
        totals = []
        for h in range(2):
            sums = [None] * 3
            for t in range(4 * h, 4 * h + 4):
                for i in range(3):
                    for c in range(3):
                        part = mx[3 * i + c, tiles[t][0], tiles[t][1]] * near[t][c]
                        sums[i] = part if sums[i] is None else sums[i] + part
            totals += [jnp.sum(s, axis=0, keepdims=True) for s in sums]
            totals.append(jnp.zeros((1, LANES), F32))
        current = KEEP * current + first + weight * jnp.concatenate(totals, axis=0)
        cbuf[n + 1, member] = current
        mine = cbuf.at[n + 1, member]
        for k in reversed(range(1, CUBE)):
            send(mine, mine, sweep_send.at[n], sweep_recv.at[n, k], cube_peers[k - 1])
        return current

    last = lax.fori_loop(1, CSWEEPS - 1, lambda n, current: sweep(n, current, True), sweep(0, first, False))

    found = coarse_values(CSWEEPS - 1, [lambda t=t: idx_v[pl.ds(8 * t, 8), :] for t in range(2)], True)
    for n in range(WIDE):
        for c in range(3):
            f3[pl.ds(c, 1), cols(n)] = f2[pl.ds(c, 1), cols(n)] + found[n // 8][c][n % 8 : n % 8 + 1, :]

    def smooth(old, n, count):
        here = cols(n - SIDE, count)
        return KEEP * old[:, cols(n, count)] + f1[values, here] + f1[weights_at, here] * y_v[:, here]

    couple_fine(border, lambda c, n: f3[pl.ds(c, 1), cols(n)])
    for n in (SIDE, BLOCKS):
        f4[:, cols(n, SIDE)] = smooth(f3, n, SIDE)
    start_sides(2)
    couple_fine(middle, lambda c, n: f3[pl.ds(c, 1), cols(n)])
    f4[:, cols(2 * SIDE, BLOCKS - 2 * SIDE)] = smooth(f3, 2 * SIDE, BLOCKS - 2 * SIDE)
    couple_fine(middle, lambda c, n: f4[pl.ds(c, 1), cols(n)])

    part = jnp.where(group_high == 0, last[0:4], last[4:8])
    moved = part
    for k in range(1, 4):
        moved = jnp.where(group_low == k, pltpu.roll(part, LANES - 32 * k, 1), moved)
    cor_o[...] = moved[0:3, 0:AGG_DEV]

    await_sides(2)
    couple_fine(border, lambda c, n: f4[pl.ds(c, 1), cols(n)])
    sol_o[...] = smooth(f4, SIDE, BLOCKS)

    for n in range(3):
        pl.when(has_right)(rightward[n].wait_send)
        pl.when(has_left)(leftward[n].wait_send)
    for n, (ref, count) in enumerate(((far0, DEVICES), (rm, GROUPS), (far1, DEVICES))):
        wait_bytes(ref.at[pl.ds(0, count - 1)], far_send.at[n])
    for n in range(CSWEEPS - 1):
        wait_bytes(cbuf.at[n + 1, pl.ds(0, CUBE - 1)], sweep_send.at[n])


def body(b, d, q, a, agg, row, cd, cq, ca):
    any_spec = pl.BlockSpec(memory_space=pl.ANY)
    vmem = pl.BlockSpec(memory_space=pltpu.VMEM)
    dma = pltpu.SemaphoreType.DMA
    sol, cor = pl.pallas_call(
        kernel,
        out_shape=(
            jax.ShapeDtypeStruct((3, NODE_DEV), F32),
            jax.ShapeDtypeStruct((3, AGG_DEV), F32),
        ),
        in_specs=[any_spec] * 9,
        out_specs=(vmem, vmem),
        scratch_shapes=[
            pltpu.VMEM((3, NODE_DEV), F32),
            pltpu.VMEM((3, NODE_DEV), F32),
            pltpu.VMEM((NNZ, NODE_DEV), I32),
            pltpu.VMEM((3, 3, NNZ, NODE_DEV), F32),
            pltpu.VMEM((BLOCKS, LANES), I32),
            pltpu.VMEM((1, AGG_DEV), I32),
            pltpu.VMEM((3, AGG_DEV), F32),
            pltpu.VMEM((AGG_DEV, NNZ), I32),
            pltpu.VMEM((3, 3, AGG_DEV, NNZ), F32),
            pltpu.VMEM((32, NODE_DEV), I32),
            pltpu.VMEM((3, NODE_DEV), F32),
            pltpu.VMEM((8, NODE_DEV), F32),
            pltpu.VMEM((LANES, NODE_DEV), BF16),
            pltpu.VMEM((16, LANES), I32),
            pltpu.VMEM((8, NODE_DEV), F32),
            pltpu.VMEM((8, WIN), F32),
            pltpu.VMEM((8, WIN), F32),
            pltpu.VMEM((3, WIDE * LANES), F32),
            pltpu.VMEM((3, WIDE * LANES), F32),
            pltpu.VMEM((3, WIDE * LANES), F32),
            pltpu.VMEM((4, LANES), F32),
            pltpu.VMEM((DEVICES, 1, LANES), F32),
            pltpu.VMEM((DEVICES, 1, LANES), F32),
            pltpu.VMEM((4, CROWS, LANES), F32),
            pltpu.VMEM((3, CROWS, LANES), F32),
            pltpu.VMEM((3, LANES, LANES), F32),
            pltpu.VMEM((GROUPS, 96, LANES), F32),
            pltpu.VMEM((9, 32, 2 * LANES), F32),
            pltpu.VMEM((32, 2 * LANES), I32),
            pltpu.VMEM((CROWS, LANES), I32),
            pltpu.VMEM((CUBE, 8, LANES), F32),
            pltpu.VMEM((CSWEEPS, CUBE, 8, LANES), F32),
            dma((9,)),
            dma((3, 2)),
            dma((3, 2)),
            pltpu.SemaphoreType.REGULAR,
            dma((3,)),
            dma((3,)),
            dma((CSWEEPS - 1,)),
            dma((CSWEEPS - 1, CUBE)),
        ],
        compiler_params=pltpu.CompilerParams(collective_id=0, has_side_effects=True),
        name="vcycle",
    )(
        b.T,
        d.T,
        q.T,
        a.transpose(2, 3, 1, 0),
        agg.reshape(BLOCKS, LANES),
        row.reshape(1, AGG_DEV),
        cd.T,
        cq,
        ca.transpose(2, 3, 0, 1),
    )
    return sol.T, cor.T


def solution(mesh):
    rows, line = P("dom", None), P("dom")
    blocks = P("dom", None, None, None)
    return jax.shard_map(
        body,
        mesh=mesh,
        in_specs=(rows, rows, rows, blocks, line, line, rows, rows, blocks),
        out_specs=(rows, rows),
        check_vma=False,
    )
```

```python
import jax
import jax.numpy as jnp
from jax import lax
from jax.experimental import pallas as pl
from jax.experimental.pallas import tpu as pltpu
from jax.sharding import PartitionSpec as P

DEVICES = 128
NODE_DEV = 1024
WIN = 256
NNZ = 27
AGG_DEV = 32
CSWEEPS = 6
LANES = 128
BLOCKS = NODE_DEV // LANES
SIDE = WIN // LANES
WIDE = BLOCKS + 2 * SIDE
REACH = 2 * SIDE + 1
CUBE = 16
GROUPS = 8
CROWS = 32
DAMP = 0.7
KEEP = 1.0 - DAMP
CUBE_BITS = ((0,), (1,), (3,), (5,))
GROUP_BITS = ((1, 2), (3, 4), (5, 6))
MESH = pl.DeviceIdType.MESH
F32, I32, BF16 = jnp.float32, jnp.int32, jnp.bfloat16


def position_of(row):
    def bit(p):
        return (row >> p) & 1

    high = (bit(10) ^ bit(11)) * 16 + (bit(8) ^ bit(9)) * 8 + (bit(6) ^ bit(7)) * 4 + bit(5) * 2 + bit(11)
    lane = bit(9) * 64 + bit(7) * 32 + (row & 31)
    return high * LANES + lane


def spread(row):
    return jnp.broadcast_to(row, (8, LANES))


def pick(row, lane):
    return jnp.take_along_axis(spread(row), lane, axis=1, mode="promise_in_bounds")


def gather_rows(place, rows, count):
    high, lane = place >> 7, place & 127
    values = [None] * 3
    for r in range(count):
        hit = high == r
        for c in range(3):
            taken = pick(rows(r, c), lane)
            values[c] = taken if r == 0 else jnp.where(hit, taken, values[c])
    return values


def kernel(
    b_h, d_h, q_h, a_h, agg_h, row_h, cd_h, cq_h, ca_h,
    out_o,
    b_v, d_v, q_v, a_v, agg_v, row_v, cd_v, cq_v, ca_v,
 q_s, y_v, r_v, onehot, idx_v,
    f1, f1l, f1r, f2, f3, f4,
    stage, far0, far1, tab0, tab1,
    pack, rm, mx, mp,
    inv_v, wbuf, cbuf,
    load_sem, side_send, side_recv, entered, far_send, far_recv, sweep_send, sweep_recv,
):
    me = lax.axis_index("dom")

    def bit(p):
        return (me // (1 << p)) % 2

    member = (bit(5) + bit(6)) % 2 * 8 + (bit(3) + bit(4)) % 2 * 4 + (bit(1) + bit(2)) % 2 * 2 + bit(0)
    group = bit(6) * 4 + bit(4) * 2 + bit(2)
    group_low, group_high = bit(4) * 2 + bit(2), bit(6)

    def flipped(bits, k):
        other = me
        for n, p in enumerate(bits):
            if (k >> n) & 1:
                for q in p:
                    other = other + (1 - 2 * bit(q)) * (1 << q)
        return other

    def ring(low, high):
        at = bit(high) * 2 + bit(low)
        places = [(at + k) % 4 for k in range(4)]
        return [(v // 2) * (1 << high) + (v % 2) * (1 << low) for v in places]

    along_x, along_z, along_y = ring(1, 2), ring(3, 4), ring(5, 6)
    cores = [bit(0), 1 - bit(0)]
    steps = [(x, z, y, c) for x in range(4) for z in range(4) for y in range(4) for c in range(2)]
    hops = (0, 1, 2, 1)
    steps = sorted(steps, key=lambda v: -(hops[v[0]] + hops[v[1]] + hops[v[2]]) - 0.5 * v[3])
    all_peers = [along_x[x] + along_z[z] + along_y[y] + cores[c] for x, z, y, c in steps if (x, z, y, c) != (0, 0, 0, 0)]
    my_high = member * 2 + bit(6)
    my_slot = ((my_high // 8) * 4 + group_low) * 8 + my_high % 8
    cube_peers = [flipped(CUBE_BITS, k) for k in range(1, CUBE)]
    group_peers = [flipped(GROUP_BITS, k) for k in range(1, GROUPS)]
    left, right = (me + DEVICES - 1) % DEVICES, (me + 1) % DEVICES

    loads = []
    for n, (src, dst) in enumerate(
        (
            (b_h, b_v), (d_h, d_v), (agg_h, agg_v), (row_h, row_v), (cd_h, cd_v),
            (cq_h, cq_v), (ca_h, ca_v), (q_h, q_v), (a_h, a_v),
        )
    ):
        copy = pltpu.make_async_copy(src, dst, load_sem.at[n])
        copy.start()
        loads.append(copy)

    barrier = pltpu.get_barrier_semaphore()
    for peer in cube_peers + group_peers + [left, right]:
        pl.semaphore_signal(barrier, inc=1, device_id=(peer,), device_id_type=MESH)

    def send(src, dst, send_sem, recv_sem, peer):
        pltpu.make_async_remote_copy(
            src_ref=src, dst_ref=dst, send_sem=send_sem, recv_sem=recv_sem,
            device_id=(peer,), device_id_type=MESH,
        ).start()

    def wait_bytes(ref, sem):
        pltpu.make_async_copy(ref, ref, sem).wait()

    lane = lax.broadcasted_iota(I32, (1, LANES), 1)

    def cols(n, count=1):
        return pl.ds(n * LANES, count * LANES)

    for n in range(4):
        loads[n].wait()
    place_row = position_of(row_v[...])
    stage[...] = jnp.zeros_like(stage)
    stage[pl.ds(3, 1), pl.ds(0, AGG_DEV)] = place_row.astype(F32)
    node_place = pick(stage[pl.ds(3, 1), :], agg_v[...])
    w0 = DAMP / d_v[...]
    f1[pl.ds(0, 3), :] = w0 * b_v[...]
    f1[pl.ds(4, 3), :] = w0
    for n in range(BLOCKS):
        f1[pl.ds(3, 1), cols(n)] = node_place[n : n + 1, :]
    pl.semaphore_wait(barrier, CUBE - 1 + GROUPS - 1 + 2)

    def to_right(n, src, dst):
        return pltpu.make_async_remote_copy(
            src_ref=src, dst_ref=dst, send_sem=side_send.at[n, 0], recv_sem=side_recv.at[n, 0],
            device_id=(right,), device_id_type=MESH,
        )

    def to_left(n, src, dst):
        return pltpu.make_async_remote_copy(
            src_ref=src, dst_ref=dst, send_sem=side_send.at[n, 1], recv_sem=side_recv.at[n, 1],
            device_id=(left,), device_id_type=MESH,
        )

    own_end, own_start = pl.ds(NODE_DEV, WIN), pl.ds(WIN, WIN)
    from_left, from_right = pl.ds(0, WIN), pl.ds(NODE_DEV + WIN, WIN)
    rightward = [
        to_right(0, f1.at[:, pl.ds(NODE_DEV - WIN, WIN)], f1l),
        to_right(1, f2.at[:, own_end], f2.at[:, from_left]),
        to_right(2, f4.at[:, own_end], f4.at[:, from_left]),
    ]
    leftward = [
        to_left(0, f1.at[:, pl.ds(0, WIN)], f1r),
        to_left(1, f2.at[:, own_start], f2.at[:, from_right]),
        to_left(2, f4.at[:, own_start], f4.at[:, from_right]),
    ]
    has_left, has_right = me > 0, me < DEVICES - 1

    def start_sides(n):
        pl.when(has_right)(rightward[n].start)
        pl.when(has_left)(leftward[n].start)

    def await_sides(n):
        pl.when(has_left)(rightward[n].wait_recv)
        pl.when(has_right)(leftward[n].wait_recv)

    start_sides(0)
    for peer in group_peers:
        pl.semaphore_signal(entered, inc=1, device_id=(peer,), device_id_type=MESH)

    for n in range(4, 9):
        loads[n].wait()
    stage[pl.ds(0, 3), pl.ds(0, AGG_DEV)] = cd_v[...]
    own = stage[...]
    line = own[0:1]
    for n in range(1, 4):
        line = jnp.where(lane // AGG_DEV == n, pltpu.roll(own, 32 * n, 1)[n : n + 1], line)
    far0[my_slot] = line

    def send_group(n, ref):
        for peer in group_peers:
            send(ref.at[group], ref.at[group], far_send.at[n], far_recv.at[n], peer)

    def send_all(n, ref):
        for peer in all_peers:
            send(ref.at[my_slot], ref.at[my_slot], far_send.at[n], far_recv.at[n], peer)

    def receive_all(n, ref, table):
        wait_bytes(ref.at[pl.ds(0, DEVICES - 1)], far_recv.at[n])
        for t in range(4):
            parts = [ref[pl.ds(32 * t + 8 * j, 8), 0, :] for j in range(4)]
            for c in range(table.shape[0]):
                whole = None
                for j in range(4):
                    moved = parts[j] if j == c else pltpu.roll(parts[j], 32 * ((j - c) % 4), 1)
                    whole = moved if j == 0 else jnp.where((lane // 32) == j, moved, whole)
                table[c, pl.ds(8 * t, 8), :] = whole

    def number_columns(n, carry):
        here = pl.ds(pl.multiple_of(n * LANES, LANES), LANES)
        q_s[pl.ds(24, 8), here] = jnp.zeros((8, LANES), I32)
        q_s[pl.ds(0, NNZ), here] = q_v[:, here] - (me * NODE_DEV - WIN + n * LANES)
        return carry

    def pack_one(e, carry):
        pack[e // 4, pl.ds(pl.multiple_of(32 * (e % 4), 32), 32), pl.ds(0, NNZ)] = ca_v[e // 3, e % 3]
        return carry

    pack[...] = jnp.zeros_like(pack)
    lax.fori_loop(0, 9, pack_one, 0)
    pack[2, pl.ds(32, 32), pl.ds(0, NNZ)] = position_of(cq_v[...]).astype(F32)
    for n in range(3):
        rm[group, pl.ds(32 * n, 32), :] = pack[n].T[0:32, :]

    lax.fori_loop(0, BLOCKS, number_columns, 0)

    def label_block(n, carry):
        label = lax.broadcasted_iota(I32, (LANES, LANES), 0) % AGG_DEV
        hit = agg_v[pl.ds(n, 1), :] == label
        onehot[:, pl.ds(pl.multiple_of(n * LANES, LANES), LANES)] = hit.astype(F32).astype(BF16)
        return carry

    lax.fori_loop(0, BLOCKS, label_block, 0)

    def couple_fine(blocks, field):
        for n in blocks:
            here = cols(n - SIDE)
            sums = [None] * 3
            for k in range(4):
                near = gather_rows(q_s[pl.ds(8 * k, 8), here], lambda r, c: field(c, n + r - SIDE), REACH)
                width = min(8, NNZ - 8 * k)
                for i in range(3):
                    term = None
                    for c in range(3):
                        part = a_v[i, c, pl.ds(8 * k, width), here] * near[c][:width]
                        term = part if term is None else term + part
                    term = jnp.sum(term, axis=0, keepdims=True) if width < 8 else term
                    if k == 0:
                        sums[i] = term
                    elif width == 8:
                        sums[i] = sums[i] + term
                    else:
                        sums[i] = jnp.sum(sums[i], axis=0, keepdims=True) + term
            for i in range(3):
                y_v[pl.ds(i, 1), here] = sums[i]

    def first_field(row, n, count=1):
        if n < SIDE:
            return f1l[row, cols(n, count)]
        if n < SIDE + BLOCKS:
            return f1[row, cols(n - SIDE, count)]
        return f1r[row, cols(n - SIDE - BLOCKS, count)]

    def start_field(c, n):
        return first_field(pl.ds(c, 1), n)

    middle = range(2 * SIDE, BLOCKS)
    border = [*range(SIDE, 2 * SIDE), *range(BLOCKS, BLOCKS + SIDE)]
    values, weights_at = pl.ds(0, 3), pl.ds(4, 3)

    couple_fine(middle, start_field)

    await_sides(0)
    couple_fine(border, start_field)
    inside = cols(SIDE, BLOCKS)
    f2[:, inside] = (1.0 + KEEP) * f1[values, :] + f1[weights_at, :] * y_v[...]
    start_sides(1)
    pl.semaphore_wait(entered, GROUPS - 1)
    send_all(0, far0)
    send_group(1, rm)
    couple_fine(middle, lambda c, n: f2[pl.ds(c, 1), cols(n)])

    r_v[...] = jnp.zeros_like(r_v)
    await_sides(1)
    couple_fine(border, lambda c, n: f2[pl.ds(c, 1), cols(n)])
    r_v[pl.ds(0, 3), :] = b_v[...] - d_v[...] * f2[:, inside] + y_v[...]
    rest = r_v[...]
    p0 = rest.astype(BF16).astype(F32)
    rest = rest - p0
    p1 = rest.astype(BF16).astype(F32)
    pieces = jnp.concatenate([p0, p1, rest - p1], axis=0).astype(BF16)
    sums = lax.dot_general(pieces, onehot[...], (((1,), (1,)), ((), ())), preferred_element_type=F32)
    sums = sums[0:4] + sums[8:12] + sums[16:20]
    line = sums[0:1]
    for n in range(1, 3):
        line = jnp.where(lane // AGG_DEV == n, sums[n : n + 1], line)
    far1[my_slot] = line
    send_all(2, far1)

    receive_all(0, far0, tab0)
    inverse = None
    for r in range(CROWS):
        place = tab0[3, pl.ds(r, 1), :].astype(I32)
        high, low = place >> 7, place & 127
        at_high = lax.broadcasted_iota(I32, (CROWS, LANES), 0) == high
        at_low = (lax.broadcasted_iota(I32, (LANES, LANES), 0) == low).astype(F32).astype(BF16)
        weights = jnp.concatenate(
            [
                jnp.where(at_high, jnp.float32(r), 0.0),
                jnp.where(at_high, lane.astype(F32), 0.0),
            ],
            axis=0,
        ).astype(BF16)
        term = lax.dot_general(weights, at_low, (((1,), (1,)), ((), ())), preferred_element_type=F32)
        inverse = term if inverse is None else inverse + term
    inv_v[...] = (inverse[0:CROWS] * LANES + inverse[CROWS : 2 * CROWS]).astype(I32)
    for c in range(3):
        tab0[c] = DAMP / tab0[c]
    for r in range(CROWS):
        for c in range(3):
            wbuf[r // 2, pl.ds(4 * (r % 2) + c, 1), :] = tab0[c, pl.ds(r, 1), :]
    wait_bytes(rm.at[pl.ds(0, GROUPS - 1)], far_recv.at[1])
    for h in range(2):
        for e4 in range(3):
            for k in range(4):
                parts = [rm[4 * h + j, pl.ds(32 * e4 + 8 * k, 8), :] for j in range(4)]
                for s in range(4):
                    e = 4 * e4 + s
                    if e > 9:
                        continue
                    whole = None
                    for j in range(4):
                        moved = parts[j] if j == s else pltpu.roll(parts[j], 32 * ((j - s) % 4), 1)
                        whole = moved if j == 0 else jnp.where((lane // 32) == j, moved, whole)
                    rows, lines = pl.ds(8 * k, 8), pl.ds(LANES * h, LANES)
                    if e < 9:
                        mx[e, rows, lines] = whole
                    else:
                        mp[rows, lines] = whole.astype(I32)

    idx_v[...] = jnp.zeros_like(idx_v)
    for n in range(WIDE):
        idx_v[pl.ds(n, 1), :] = first_field(pl.ds(3, 1), n).astype(I32)

    receive_all(2, far1, tab1)

    for t in range(CROWS // 8):
        sums = gather_rows(inv_v[pl.ds(8 * t, 8), :], lambda r, c: tab1[c, pl.ds(r, 1), :], CROWS)
        for c in range(3):
            value = sums[c] * tab0[c, pl.ds(8 * t, 8), :]
            for n in range(8):
                r = 8 * t + n
                cbuf[0, r // 2, pl.ds(4 * (r % 2) + c, 1), :] = value[n : n + 1, :]

    unused = lax.broadcasted_iota(I32, (8, LANES), 0) % 4 == 3
    first = jnp.where(unused, 0.0, cbuf[0, member])
    weight = jnp.where(unused, 0.0, wbuf[member])

    def place(k):
        slot = member
        for p, w in enumerate((1, 2, 4, 8)):
            if (k >> p) & 1:
                slot = slot + (1 - 2 * ((member // w) % 2)) * w
        return slot

    stages = [[k for k in range(CUBE) if bin(k >> 1).count("1") == hops] for hops in range(4)]

    def coarse_values(n, places, arrive):
        found = [[jnp.zeros((8, LANES), F32)] * 3 for _ in places]
        for stage_of in stages:
            for k in stage_of:
                if k and arrive:
                    there = cbuf.at[n, place(k)]
                    pltpu.make_async_copy(there, there, sweep_recv.at[n - 1, k]).wait()
            for t, where in enumerate(places):
                high, low = where() >> 7, where() & 127
                for k in stage_of:
                    slot = place(k)
                    for h in range(2):
                        hit = high == slot * 2 + h
                        for c in range(3):
                            taken = pick(cbuf[n, slot, pl.ds(4 * h + c, 1), :], low)
                            found[t][c] = jnp.where(hit, taken, found[t][c])
        return found

    tiles = [(pl.ds(8 * k, 8), pl.ds(LANES * h, LANES)) for h in range(2) for k in range(4)]

    def sweep(n, current, arrive):
        near = coarse_values(n, [lambda at=at: mp[at] for at in tiles], arrive)
        totals = []
        for h in range(2):
            sums = [None] * 3
            for t in range(4 * h, 4 * h + 4):
                for i in range(3):
                    for c in range(3):
                        part = mx[3 * i + c, tiles[t][0], tiles[t][1]] * near[t][c]
                        sums[i] = part if sums[i] is None else sums[i] + part
            totals += [jnp.sum(s, axis=0, keepdims=True) for s in sums]
            totals.append(jnp.zeros((1, LANES), F32))
        current = KEEP * current + first + weight * jnp.concatenate(totals, axis=0)
        cbuf[n + 1, member] = current
        mine = cbuf.at[n + 1, member]
        for k in reversed(range(1, CUBE)):
            send(mine, mine, sweep_send.at[n], sweep_recv.at[n, k], cube_peers[k - 1])
        return current

    last = lax.fori_loop(1, CSWEEPS - 1, lambda n, current: sweep(n, current, True), sweep(0, first, False))

    found = coarse_values(CSWEEPS - 1, [lambda t=t: idx_v[pl.ds(8 * t, 8), :] for t in range(2)], True)
    for n in range(WIDE):
        for c in range(3):
            f3[pl.ds(c, 1), cols(n)] = f2[pl.ds(c, 1), cols(n)] + found[n // 8][c][n % 8 : n % 8 + 1, :]

    def smooth(old, n, count):
        here = cols(n - SIDE, count)
        return KEEP * old[:, cols(n, count)] + f1[values, here] + f1[weights_at, here] * y_v[:, here]

    couple_fine(border, lambda c, n: f3[pl.ds(c, 1), cols(n)])
    for n in (SIDE, BLOCKS):
        f4[:, cols(n, SIDE)] = smooth(f3, n, SIDE)
    start_sides(2)
    couple_fine(middle, lambda c, n: f3[pl.ds(c, 1), cols(n)])
    f4[:, cols(2 * SIDE, BLOCKS - 2 * SIDE)] = smooth(f3, 2 * SIDE, BLOCKS - 2 * SIDE)
    couple_fine(middle, lambda c, n: f4[pl.ds(c, 1), cols(n)])

    part = jnp.where(group_high == 0, last[0:4], last[4:8])
    moved = part
    for k in range(1, 4):
        moved = jnp.where(group_low == k, pltpu.roll(part, LANES - 32 * k, 1), moved)
    out_o[:, pl.ds(NODE_DEV, LANES)] = moved[0:3]

    await_sides(2)
    couple_fine(border, lambda c, n: f4[pl.ds(c, 1), cols(n)])
    out_o[:, pl.ds(0, NODE_DEV)] = smooth(f4, SIDE, BLOCKS)

    for n in range(3):
        pl.when(has_right)(rightward[n].wait_send)
        pl.when(has_left)(leftward[n].wait_send)
    for n, (ref, count) in enumerate(((far0, DEVICES), (rm, GROUPS), (far1, DEVICES))):
        wait_bytes(ref.at[pl.ds(0, count - 1)], far_send.at[n])
    for n in range(CSWEEPS - 1):
        wait_bytes(cbuf.at[n + 1, pl.ds(0, CUBE - 1)], sweep_send.at[n])


def split(all_ref, sol_o, cor_o):
    sol_o[...] = all_ref[:, pl.ds(0, NODE_DEV)]
    cor_o[...] = all_ref[:, pl.ds(NODE_DEV, LANES)][:, 0:AGG_DEV]


def body(b, d, q, a, agg, row, cd, cq, ca):
    any_spec = pl.BlockSpec(memory_space=pl.ANY)
    vmem = pl.BlockSpec(memory_space=pltpu.VMEM)
    dma = pltpu.SemaphoreType.DMA
    out = pl.pallas_call(
        kernel,
        out_shape=pltpu.VMEM((3, NODE_DEV + LANES), F32),
        in_specs=[any_spec] * 9,
        out_specs=vmem,
        scratch_shapes=[
            pltpu.VMEM((3, NODE_DEV), F32),
            pltpu.VMEM((3, NODE_DEV), F32),
            pltpu.VMEM((NNZ, NODE_DEV), I32),
            pltpu.VMEM((3, 3, NNZ, NODE_DEV), F32),
            pltpu.VMEM((BLOCKS, LANES), I32),
            pltpu.VMEM((1, AGG_DEV), I32),
            pltpu.VMEM((3, AGG_DEV), F32),
            pltpu.VMEM((AGG_DEV, NNZ), I32),
            pltpu.VMEM((3, 3, AGG_DEV, NNZ), F32),
            pltpu.VMEM((32, NODE_DEV), I32),
            pltpu.VMEM((3, NODE_DEV), F32),
            pltpu.VMEM((8, NODE_DEV), F32),
            pltpu.VMEM((LANES, NODE_DEV), BF16),
            pltpu.VMEM((16, LANES), I32),
            pltpu.VMEM((8, NODE_DEV), F32),
            pltpu.VMEM((8, WIN), F32),
            pltpu.VMEM((8, WIN), F32),
            pltpu.VMEM((3, WIDE * LANES), F32),
            pltpu.VMEM((3, WIDE * LANES), F32),
            pltpu.VMEM((3, WIDE * LANES), F32),
            pltpu.VMEM((4, LANES), F32),
            pltpu.VMEM((DEVICES, 1, LANES), F32),
            pltpu.VMEM((DEVICES, 1, LANES), F32),
            pltpu.VMEM((4, CROWS, LANES), F32),
            pltpu.VMEM((3, CROWS, LANES), F32),
            pltpu.VMEM((3, LANES, LANES), F32),
            pltpu.VMEM((GROUPS, 96, LANES), F32),
            pltpu.VMEM((9, 32, 2 * LANES), F32),
            pltpu.VMEM((32, 2 * LANES), I32),
            pltpu.VMEM((CROWS, LANES), I32),
            pltpu.VMEM((CUBE, 8, LANES), F32),
            pltpu.VMEM((CSWEEPS, CUBE, 8, LANES), F32),
            dma((9,)),
            dma((3, 2)),
            dma((3, 2)),
            pltpu.SemaphoreType.REGULAR,
            dma((3,)),
            dma((3,)),
            dma((CSWEEPS - 1,)),
            dma((CSWEEPS - 1, CUBE)),
        ],
        compiler_params=pltpu.CompilerParams(collective_id=0, has_side_effects=True),
        name="vcycle",
    )(
        b.T,
        d.T,
        q.T,
        a.transpose(2, 3, 1, 0),
        agg.reshape(BLOCKS, LANES),
        row.reshape(1, AGG_DEV),
        cd.T,
        cq,
        ca.transpose(2, 3, 0, 1),
    )
    sol, cor = pl.pallas_call(
        split,
        out_shape=(
            jax.ShapeDtypeStruct((3, NODE_DEV), F32),
            jax.ShapeDtypeStruct((3, AGG_DEV), F32),
        ),
        in_specs=[vmem],
        out_specs=(vmem, vmem),
        name="split",
    )(pltpu.with_memory_space_constraint(out, pltpu.VMEM))
    return sol.T, cor.T


def solution(mesh):
    rows, line = P("dom", None), P("dom")
    blocks = P("dom", None, None, None)
    return jax.shard_map(
        body,
        mesh=mesh,
        in_specs=(rows, rows, rows, blocks, line, line, rows, rows, blocks),
        out_specs=(rows, rows),
        check_vma=False,
    )
```

```python
import jax
import jax.numpy as jnp
from jax import lax
from jax.experimental import pallas as pl
from jax.experimental.pallas import tpu as pltpu
from jax.sharding import PartitionSpec as P

DEVICES = 128
NODE_DEV = 1024
WIN = 256
NNZ = 27
AGG_DEV = 32
CSWEEPS = 6
LANES = 128
BLOCKS = NODE_DEV // LANES
SIDE = WIN // LANES
WIDE = BLOCKS + 2 * SIDE
REACH = 2 * SIDE + 1
CUBE = 16
GROUPS = 8
CROWS = 32
DAMP = 0.7
KEEP = 1.0 - DAMP
CUBE_BITS = ((0,), (1,), (3,), (5,))
GROUP_BITS = ((1, 2), (3, 4), (5, 6))
MESH = pl.DeviceIdType.MESH
F32, I32, BF16 = jnp.float32, jnp.int32, jnp.bfloat16


def position_of(row):
    def bit(p):
        return (row >> p) & 1

    high = (bit(10) ^ bit(11)) * 16 + (bit(8) ^ bit(9)) * 8 + (bit(6) ^ bit(7)) * 4 + bit(5) * 2 + bit(11)
    lane = bit(9) * 64 + bit(7) * 32 + (row & 31)
    return high * LANES + lane


def spread(row):
    return jnp.broadcast_to(row, (8, LANES))


def pick(row, lane):
    return jnp.take_along_axis(spread(row), lane, axis=1, mode="promise_in_bounds")


def gather_rows(place, rows, count):
    high, lane = place >> 7, place & 127
    values = [None] * 3
    for r in range(count):
        hit = high == r
        for c in range(3):
            taken = pick(rows(r, c), lane)
            values[c] = taken if r == 0 else jnp.where(hit, taken, values[c])
    return values


def kernel(
    b_h, d_h, q_h, a_h, agg_h, row_h, cd_h, cq_h, ca_h,
    out_o,
    b_v, d_v, q_v, a_v, agg_v, row_v, cd_v, cq_v, ca_v,
 q_s, y_v, r_v, onehot, idx_v,
    f1, f1l, f1r, f2, f3, f4,
    stage, far0, far1, tab0, tab1,
    pack, rm, mx, mp,
    inv_v, wbuf, cbuf,
    load_sem, side_send, side_recv, entered, far_send, far_recv, sweep_send, sweep_recv,
):
    me = lax.axis_index("dom")

    def bit(p):
        return (me // (1 << p)) % 2

    member = (bit(5) + bit(6)) % 2 * 8 + (bit(3) + bit(4)) % 2 * 4 + (bit(1) + bit(2)) % 2 * 2 + bit(0)
    group = bit(6) * 4 + bit(4) * 2 + bit(2)
    group_low, group_high = bit(4) * 2 + bit(2), bit(6)

    def flipped(bits, k):
        other = me
        for n, p in enumerate(bits):
            if (k >> n) & 1:
                for q in p:
                    other = other + (1 - 2 * bit(q)) * (1 << q)
        return other

    def ring(low, high):
        at = bit(high) * 2 + bit(low)
        places = [(at + k) % 4 for k in range(4)]
        return [(v // 2) * (1 << high) + (v % 2) * (1 << low) for v in places]

    along_x, along_z, along_y = ring(1, 2), ring(3, 4), ring(5, 6)
    cores = [bit(0), 1 - bit(0)]
    steps = [(x, z, y, c) for x in range(4) for z in range(4) for y in range(4) for c in range(2)]
    hops = (0, 1, 2, 1)
    steps = sorted(steps, key=lambda v: -(hops[v[0]] + hops[v[1]] + hops[v[2]]) - 0.5 * v[3])
    all_peers = [along_x[x] + along_z[z] + along_y[y] + cores[c] for x, z, y, c in steps if (x, z, y, c) != (0, 0, 0, 0)]
    my_high = member * 2 + bit(6)
    my_slot = ((my_high // 8) * 4 + group_low) * 8 + my_high % 8
    cube_peers = [flipped(CUBE_BITS, k) for k in range(1, CUBE)]
    group_peers = [flipped(GROUP_BITS, k) for k in range(1, GROUPS)]
    left, right = (me + DEVICES - 1) % DEVICES, (me + 1) % DEVICES

    loads = []
    for n, (src, dst) in enumerate(
        (
            (b_h, b_v), (d_h, d_v), (agg_h, agg_v), (row_h, row_v), (cd_h, cd_v),
            (cq_h, cq_v), (ca_h, ca_v), (q_h, q_v), (a_h, a_v),
        )
    ):
        copy = pltpu.make_async_copy(src, dst, load_sem.at[n])
        copy.start()
        loads.append(copy)

    barrier = pltpu.get_barrier_semaphore()
    beside = [group_peers[k - 1] for k in (1, 2, 4)]
    for peer in cube_peers + beside + [left, right]:
        pl.semaphore_signal(barrier, inc=1, device_id=(peer,), device_id_type=MESH)

    def send(src, dst, send_sem, recv_sem, peer):
        pltpu.make_async_remote_copy(
            src_ref=src, dst_ref=dst, send_sem=send_sem, recv_sem=recv_sem,
            device_id=(peer,), device_id_type=MESH,
        ).start()

    def wait_bytes(ref, sem):
        pltpu.make_async_copy(ref, ref, sem).wait()

    lane = lax.broadcasted_iota(I32, (1, LANES), 1)

    def cols(n, count=1):
        return pl.ds(n * LANES, count * LANES)

    for n in range(4):
        loads[n].wait()
    place_row = position_of(row_v[...])
    stage[...] = jnp.zeros_like(stage)
    stage[pl.ds(3, 1), pl.ds(0, AGG_DEV)] = place_row.astype(F32)
    node_place = pick(stage[pl.ds(3, 1), :], agg_v[...])
    w0 = DAMP / d_v[...]
    f1[pl.ds(0, 3), :] = w0 * b_v[...]
    f1[pl.ds(4, 3), :] = w0
    for n in range(BLOCKS):
        f1[pl.ds(3, 1), cols(n)] = node_place[n : n + 1, :]
    pl.semaphore_wait(barrier, CUBE - 1 + 3 + 2)

    def to_right(n, src, dst):
        return pltpu.make_async_remote_copy(
            src_ref=src, dst_ref=dst, send_sem=side_send.at[n, 0], recv_sem=side_recv.at[n, 0],
            device_id=(right,), device_id_type=MESH,
        )

    def to_left(n, src, dst):
        return pltpu.make_async_remote_copy(
            src_ref=src, dst_ref=dst, send_sem=side_send.at[n, 1], recv_sem=side_recv.at[n, 1],
            device_id=(left,), device_id_type=MESH,
        )

    own_end, own_start = pl.ds(NODE_DEV, WIN), pl.ds(WIN, WIN)
    from_left, from_right = pl.ds(0, WIN), pl.ds(NODE_DEV + WIN, WIN)
    rightward = [
        to_right(0, f1.at[:, pl.ds(NODE_DEV - WIN, WIN)], f1l),
        to_right(1, f2.at[:, own_end], f2.at[:, from_left]),
        to_right(2, f4.at[:, own_end], f4.at[:, from_left]),
    ]
    leftward = [
        to_left(0, f1.at[:, pl.ds(0, WIN)], f1r),
        to_left(1, f2.at[:, own_start], f2.at[:, from_right]),
        to_left(2, f4.at[:, own_start], f4.at[:, from_right]),
    ]
    has_left, has_right = me > 0, me < DEVICES - 1

    def start_sides(n):
        pl.when(has_right)(rightward[n].start)
        pl.when(has_left)(leftward[n].start)

    def await_sides(n):
        pl.when(has_left)(rightward[n].wait_recv)
        pl.when(has_right)(leftward[n].wait_recv)

    start_sides(0)

    def tell(n):
        pl.semaphore_signal(entered.at[n], inc=1, device_id=(beside[n],), device_id_type=MESH)

    tell(0)

    for n in range(4, 9):
        loads[n].wait()
    stage[pl.ds(0, 3), pl.ds(0, AGG_DEV)] = cd_v[...]
    own = stage[...]
    line = own[0:1]
    for n in range(1, 4):
        line = jnp.where(lane // AGG_DEV == n, pltpu.roll(own, 32 * n, 1)[n : n + 1], line)
    far0[my_slot] = line

    def send_group(n, ref):
        for peer in group_peers:
            send(ref.at[group], ref.at[group], far_send.at[n], far_recv.at[n], peer)

    def send_all(n, ref):
        for peer in all_peers:
            send(ref.at[my_slot], ref.at[my_slot], far_send.at[n], far_recv.at[n], peer)

    def receive_all(n, ref, table):
        wait_bytes(ref.at[pl.ds(0, DEVICES - 1)], far_recv.at[n])
        for t in range(4):
            parts = [ref[pl.ds(32 * t + 8 * j, 8), 0, :] for j in range(4)]
            for c in range(table.shape[0]):
                whole = None
                for j in range(4):
                    moved = parts[j] if j == c else pltpu.roll(parts[j], 32 * ((j - c) % 4), 1)
                    whole = moved if j == 0 else jnp.where((lane // 32) == j, moved, whole)
                table[c, pl.ds(8 * t, 8), :] = whole

    def number_columns(n, carry):
        here = pl.ds(pl.multiple_of(n * LANES, LANES), LANES)
        q_s[pl.ds(24, 8), here] = jnp.zeros((8, LANES), I32)
        q_s[pl.ds(0, NNZ), here] = q_v[:, here] - (me * NODE_DEV - WIN + n * LANES)
        return carry

    def pack_one(e, carry):
        pack[e // 4, pl.ds(pl.multiple_of(32 * (e % 4), 32), 32), pl.ds(0, NNZ)] = ca_v[e // 3, e % 3]
        return carry

    pack[...] = jnp.zeros_like(pack)
    lax.fori_loop(0, 9, pack_one, 0)
    pack[2, pl.ds(32, 32), pl.ds(0, NNZ)] = position_of(cq_v[...]).astype(F32)
    for n in range(3):
        rm[group, pl.ds(32 * n, 32), :] = pack[n].T[0:32, :]

    lax.fori_loop(0, BLOCKS, number_columns, 0)

    def label_block(n, carry):
        label = lax.broadcasted_iota(I32, (LANES, LANES), 0) % AGG_DEV
        hit = agg_v[pl.ds(n, 1), :] == label
        onehot[:, pl.ds(pl.multiple_of(n * LANES, LANES), LANES)] = hit.astype(F32).astype(BF16)
        return carry

    lax.fori_loop(0, BLOCKS, label_block, 0)

    def couple_fine(blocks, field):
        for n in blocks:
            here = cols(n - SIDE)
            sums = [None] * 3
            for k in range(4):
                near = gather_rows(q_s[pl.ds(8 * k, 8), here], lambda r, c: field(c, n + r - SIDE), REACH)
                width = min(8, NNZ - 8 * k)
                for i in range(3):
                    term = None
                    for c in range(3):
                        part = a_v[i, c, pl.ds(8 * k, width), here] * near[c][:width]
                        term = part if term is None else term + part
                    term = jnp.sum(term, axis=0, keepdims=True) if width < 8 else term
                    if k == 0:
                        sums[i] = term
                    elif width == 8:
                        sums[i] = sums[i] + term
                    else:
                        sums[i] = jnp.sum(sums[i], axis=0, keepdims=True) + term
            for i in range(3):
                y_v[pl.ds(i, 1), here] = sums[i]

    def first_field(row, n, count=1):
        if n < SIDE:
            return f1l[row, cols(n, count)]
        if n < SIDE + BLOCKS:
            return f1[row, cols(n - SIDE, count)]
        return f1r[row, cols(n - SIDE - BLOCKS, count)]

    def start_field(c, n):
        return first_field(pl.ds(c, 1), n)

    middle = range(2 * SIDE, BLOCKS)
    border = [*range(SIDE, 2 * SIDE), *range(BLOCKS, BLOCKS + SIDE)]
    values, weights_at = pl.ds(0, 3), pl.ds(4, 3)

    pl.semaphore_wait(entered.at[0], 1)
    tell(1)
    couple_fine(middle, start_field)
    pl.semaphore_wait(entered.at[1], 1)
    tell(2)

    await_sides(0)
    couple_fine(border, start_field)
    inside = cols(SIDE, BLOCKS)
    f2[:, inside] = (1.0 + KEEP) * f1[values, :] + f1[weights_at, :] * y_v[...]
    start_sides(1)
    pl.semaphore_wait(entered.at[2], 1)
    send_all(0, far0)
    send_group(1, rm)
    couple_fine(middle, lambda c, n: f2[pl.ds(c, 1), cols(n)])

    r_v[...] = jnp.zeros_like(r_v)
    await_sides(1)
    couple_fine(border, lambda c, n: f2[pl.ds(c, 1), cols(n)])
    r_v[pl.ds(0, 3), :] = b_v[...] - d_v[...] * f2[:, inside] + y_v[...]
    rest = r_v[...]
    p0 = rest.astype(BF16).astype(F32)
    rest = rest - p0
    p1 = rest.astype(BF16).astype(F32)
    pieces = jnp.concatenate([p0, p1, rest - p1], axis=0).astype(BF16)
    sums = lax.dot_general(pieces, onehot[...], (((1,), (1,)), ((), ())), preferred_element_type=F32)
    sums = sums[0:4] + sums[8:12] + sums[16:20]
    line = sums[0:1]
    for n in range(1, 3):
        line = jnp.where(lane // AGG_DEV == n, sums[n : n + 1], line)
    far1[my_slot] = line
    send_all(2, far1)

    receive_all(0, far0, tab0)
    inverse = None
    for r in range(CROWS):
        place = tab0[3, pl.ds(r, 1), :].astype(I32)
        high, low = place >> 7, place & 127
        at_high = lax.broadcasted_iota(I32, (CROWS, LANES), 0) == high
        at_low = (lax.broadcasted_iota(I32, (LANES, LANES), 0) == low).astype(F32).astype(BF16)
        weights = jnp.concatenate(
            [
                jnp.where(at_high, jnp.float32(r), 0.0),
                jnp.where(at_high, lane.astype(F32), 0.0),
            ],
            axis=0,
        ).astype(BF16)
        term = lax.dot_general(weights, at_low, (((1,), (1,)), ((), ())), preferred_element_type=F32)
        inverse = term if inverse is None else inverse + term
    inv_v[...] = (inverse[0:CROWS] * LANES + inverse[CROWS : 2 * CROWS]).astype(I32)
    for c in range(3):
        tab0[c] = DAMP / tab0[c]
    for r in range(CROWS):
        for c in range(3):
            wbuf[r // 2, pl.ds(4 * (r % 2) + c, 1), :] = tab0[c, pl.ds(r, 1), :]
    wait_bytes(rm.at[pl.ds(0, GROUPS - 1)], far_recv.at[1])
    spare = {}
    for h in range(2):
        for e4 in range(3):
            for k in range(4):
                parts = [rm[4 * h + j, pl.ds(32 * e4 + 8 * k, 8), :] for j in range(4)]
                for s in range(4):
                    e = 4 * e4 + s
                    if e > 9:
                        continue
                    whole = None
                    for j in range(4):
                        moved = parts[j] if j == s else pltpu.roll(parts[j], 32 * ((j - s) % 4), 1)
                        whole = moved if j == 0 else jnp.where((lane // 32) == j, moved, whole)
                    rows, lines = pl.ds(8 * k, 8), pl.ds(LANES * h, LANES)
                    if k == 3:
                        lines = pl.ds(0, LANES)
                        if h == 0:
                            spare[e] = whole
                            continue
                        whole = spare[e] + pltpu.roll(whole, NNZ - 24, 0)
                    if e < 9:
                        mx[e, rows, lines] = whole
                    else:
                        mp[rows, lines] = whole.astype(I32)

    idx_v[...] = jnp.zeros_like(idx_v)
    for n in range(WIDE):
        idx_v[pl.ds(n, 1), :] = first_field(pl.ds(3, 1), n).astype(I32)

    receive_all(2, far1, tab1)

    for t in range(CROWS // 8):
        sums = gather_rows(inv_v[pl.ds(8 * t, 8), :], lambda r, c: tab1[c, pl.ds(r, 1), :], CROWS)
        for c in range(3):
            value = sums[c] * tab0[c, pl.ds(8 * t, 8), :]
            for n in range(8):
                r = 8 * t + n
                cbuf[0, r // 2, pl.ds(4 * (r % 2) + c, 1), :] = value[n : n + 1, :]

    unused = lax.broadcasted_iota(I32, (8, LANES), 0) % 4 == 3
    first = jnp.where(unused, 0.0, cbuf[0, member])
    weight = jnp.where(unused, 0.0, wbuf[member])

    def place(k):
        slot = member
        for p, w in enumerate((1, 2, 4, 8)):
            if (k >> p) & 1:
                slot = slot + (1 - 2 * ((member // w) % 2)) * w
        return slot

    stages = [[k for k in range(CUBE) if bin(k >> 1).count("1") == hops] for hops in range(4)]

    def coarse_values(n, places, arrive):
        found = [[jnp.zeros((8, LANES), F32)] * 3 for _ in places]
        for stage_of in stages:
            for k in stage_of:
                if k and arrive:
                    there = cbuf.at[n, place(k)]
                    pltpu.make_async_copy(there, there, sweep_recv.at[n - 1, k]).wait()
            for t, where in enumerate(places):
                high, low = where() >> 7, where() & 127
                for k in stage_of:
                    slot = place(k)
                    for h in range(2):
                        hit = high == slot * 2 + h
                        for c in range(3):
                            taken = pick(cbuf[n, slot, pl.ds(4 * h + c, 1), :], low)
                            found[t][c] = jnp.where(hit, taken, found[t][c])
        return found

    tiles = [(pl.ds(8 * k, 8), pl.ds(LANES * h, LANES)) for h in range(2) for k in range(3)]
    tiles.append((pl.ds(24, 8), pl.ds(0, LANES)))
    sublane = lax.broadcasted_iota(I32, (8, LANES), 0)

    def sweep(n, current, arrive):
        near = coarse_values(n, [lambda at=at: mp[at] for at in tiles], arrive)

        def product(i, which):
            total = None
            for t in which:
                for c in range(3):
                    part = mx[3 * i + c, tiles[t][0], tiles[t][1]] * near[t][c]
                    total = part if total is None else total + part
            return total

        shared = [product(i, (6,)) for i in range(3)]
        totals = []
        for h in range(2):
            for i in range(3):
                mine = sublane < NNZ - 24 if h == 0 else sublane >= NNZ - 24
                total = product(i, range(3 * h, 3 * h + 3)) + jnp.where(mine, shared[i], 0.0)
                totals.append(jnp.sum(total, axis=0, keepdims=True))
            totals.append(jnp.zeros((1, LANES), F32))
        current = KEEP * current + first + weight * jnp.concatenate(totals, axis=0)
        cbuf[n + 1, member] = current
        mine = cbuf.at[n + 1, member]
        for k in reversed(range(1, CUBE)):
            send(mine, mine, sweep_send.at[n], sweep_recv.at[n, k], cube_peers[k - 1])
        return current

    last = lax.fori_loop(1, CSWEEPS - 1, lambda n, current: sweep(n, current, True), sweep(0, first, False))

    found = coarse_values(CSWEEPS - 1, [lambda t=t: idx_v[pl.ds(8 * t, 8), :] for t in range(2)], True)
    for n in range(WIDE):
        for c in range(3):
            f3[pl.ds(c, 1), cols(n)] = f2[pl.ds(c, 1), cols(n)] + found[n // 8][c][n % 8 : n % 8 + 1, :]

    def smooth(old, n, count):
        here = cols(n - SIDE, count)
        return KEEP * old[:, cols(n, count)] + f1[values, here] + f1[weights_at, here] * y_v[:, here]

    couple_fine(border, lambda c, n: f3[pl.ds(c, 1), cols(n)])
    for n in (SIDE, BLOCKS):
        f4[:, cols(n, SIDE)] = smooth(f3, n, SIDE)
    start_sides(2)
    couple_fine(middle, lambda c, n: f3[pl.ds(c, 1), cols(n)])
    f4[:, cols(2 * SIDE, BLOCKS - 2 * SIDE)] = smooth(f3, 2 * SIDE, BLOCKS - 2 * SIDE)
    couple_fine(middle, lambda c, n: f4[pl.ds(c, 1), cols(n)])

    part = jnp.where(group_high == 0, last[0:4], last[4:8])
    moved = part
    for k in range(1, 4):
        moved = jnp.where(group_low == k, pltpu.roll(part, LANES - 32 * k, 1), moved)
    out_o[:, pl.ds(NODE_DEV, LANES)] = moved[0:3]

    await_sides(2)
    couple_fine(border, lambda c, n: f4[pl.ds(c, 1), cols(n)])
    out_o[:, pl.ds(0, NODE_DEV)] = smooth(f4, SIDE, BLOCKS)

    for n in range(3):
        pl.when(has_right)(rightward[n].wait_send)
        pl.when(has_left)(leftward[n].wait_send)
    for n, (ref, count) in enumerate(((far0, DEVICES), (rm, GROUPS), (far1, DEVICES))):
        wait_bytes(ref.at[pl.ds(0, count - 1)], far_send.at[n])
    for n in range(CSWEEPS - 1):
        wait_bytes(cbuf.at[n + 1, pl.ds(0, CUBE - 1)], sweep_send.at[n])


def split(all_ref, sol_o, cor_o):
    sol_o[...] = all_ref[:, pl.ds(0, NODE_DEV)]
    cor_o[...] = all_ref[:, pl.ds(NODE_DEV, LANES)][:, 0:AGG_DEV]


def body(b, d, q, a, agg, row, cd, cq, ca):
    any_spec = pl.BlockSpec(memory_space=pl.ANY)
    vmem = pl.BlockSpec(memory_space=pltpu.VMEM)
    dma = pltpu.SemaphoreType.DMA
    out = pl.pallas_call(
        kernel,
        out_shape=pltpu.VMEM((3, NODE_DEV + LANES), F32),
        in_specs=[any_spec] * 9,
        out_specs=vmem,
        scratch_shapes=[
            pltpu.VMEM((3, NODE_DEV), F32),
            pltpu.VMEM((3, NODE_DEV), F32),
            pltpu.VMEM((NNZ, NODE_DEV), I32),
            pltpu.VMEM((3, 3, NNZ, NODE_DEV), F32),
            pltpu.VMEM((BLOCKS, LANES), I32),
            pltpu.VMEM((1, AGG_DEV), I32),
            pltpu.VMEM((3, AGG_DEV), F32),
            pltpu.VMEM((AGG_DEV, NNZ), I32),
            pltpu.VMEM((3, 3, AGG_DEV, NNZ), F32),
            pltpu.VMEM((32, NODE_DEV), I32),
            pltpu.VMEM((3, NODE_DEV), F32),
            pltpu.VMEM((8, NODE_DEV), F32),
            pltpu.VMEM((LANES, NODE_DEV), BF16),
            pltpu.VMEM((16, LANES), I32),
            pltpu.VMEM((8, NODE_DEV), F32),
            pltpu.VMEM((8, WIN), F32),
            pltpu.VMEM((8, WIN), F32),
            pltpu.VMEM((3, WIDE * LANES), F32),
            pltpu.VMEM((3, WIDE * LANES), F32),
            pltpu.VMEM((3, WIDE * LANES), F32),
            pltpu.VMEM((4, LANES), F32),
            pltpu.VMEM((DEVICES, 1, LANES), F32),
            pltpu.VMEM((DEVICES, 1, LANES), F32),
            pltpu.VMEM((4, CROWS, LANES), F32),
            pltpu.VMEM((3, CROWS, LANES), F32),
            pltpu.VMEM((3, LANES, LANES), F32),
            pltpu.VMEM((GROUPS, 96, LANES), F32),
            pltpu.VMEM((9, 32, 2 * LANES), F32),
            pltpu.VMEM((32, 2 * LANES), I32),
            pltpu.VMEM((CROWS, LANES), I32),
            pltpu.VMEM((CUBE, 8, LANES), F32),
            pltpu.VMEM((CSWEEPS, CUBE, 8, LANES), F32),
            dma((9,)),
            dma((3, 2)),
            dma((3, 2)),
            pltpu.SemaphoreType.REGULAR((3,)),
            dma((3,)),
            dma((3,)),
            dma((CSWEEPS - 1,)),
            dma((CSWEEPS - 1, CUBE)),
        ],
        compiler_params=pltpu.CompilerParams(collective_id=0, has_side_effects=True),
        name="vcycle",
    )(
        b.T,
        d.T,
        q.T,
        a.transpose(2, 3, 1, 0),
        agg.reshape(BLOCKS, LANES),
        row.reshape(1, AGG_DEV),
        cd.T,
        cq,
        ca.transpose(2, 3, 0, 1),
    )
    sol, cor = pl.pallas_call(
        split,
        out_shape=(
            jax.ShapeDtypeStruct((3, NODE_DEV), F32),
            jax.ShapeDtypeStruct((3, AGG_DEV), F32),
        ),
        in_specs=[vmem],
        out_specs=(vmem, vmem),
        name="split",
    )(pltpu.with_memory_space_constraint(out, pltpu.VMEM))
    return sol.T, cor.T


def solution(mesh):
    rows, line = P("dom", None), P("dom")
    blocks = P("dom", None, None, None)
    return jax.shard_map(
        body,
        mesh=mesh,
        in_specs=(rows, rows, rows, blocks, line, line, rows, rows, blocks),
        out_specs=(rows, rows),
        check_vma=False,
    )
```

```python
import jax
import jax.numpy as jnp
from jax import lax
from jax.experimental import pallas as pl
from jax.experimental.pallas import tpu as pltpu
from jax.sharding import PartitionSpec as P

DEVICES = 128
NODE_DEV = 1024
WIN = 256
NNZ = 27
AGG_DEV = 32
CSWEEPS = 6
LANES = 128
BLOCKS = NODE_DEV // LANES
SIDE = WIN // LANES
WIDE = BLOCKS + 2 * SIDE
REACH = 2 * SIDE + 1
CUBE = 16
GROUPS = 8
CROWS = 32
DAMP = 0.7
KEEP = 1.0 - DAMP
CUBE_BITS = ((0,), (1,), (3,), (5,))
GROUP_BITS = ((1, 2), (3, 4), (5, 6))
MESH = pl.DeviceIdType.MESH
F32, I32, BF16 = jnp.float32, jnp.int32, jnp.bfloat16


def position_of(row):
    def bit(p):
        return (row >> p) & 1

    high = (bit(10) ^ bit(11)) * 16 + (bit(8) ^ bit(9)) * 8 + (bit(6) ^ bit(7)) * 4 + bit(5) * 2 + bit(11)
    lane = bit(9) * 64 + bit(7) * 32 + (row & 31)
    return high * LANES + lane


def spread(row):
    return jnp.broadcast_to(row, (8, LANES))


def pick(row, lane):
    return jnp.take_along_axis(spread(row), lane, axis=1, mode="promise_in_bounds")


def gather_rows(place, rows, count):
    high, lane = place >> 7, place & 127
    values = [None] * 3
    for r in range(count):
        hit = high == r
        for c in range(3):
            taken = pick(rows(r, c), lane)
            values[c] = taken if r == 0 else jnp.where(hit, taken, values[c])
    return values


def kernel(
    b_h, d_h, q_h, a_h, agg_h, row_h, cd_h, cq_h, ca_h,
    out_o,
    b_v, d_v, q_v, a_v, agg_v, row_v, cd_v, cq_v, ca_v,
 q_s, y_v, r_v, onehot, idx_v,
    f1, f1l, f1r, f2, f3, f4,
    stage, far0, far1, tab0, tab1,
    pack, rm, mx, mp,
    inv_v, wbuf, cbuf,
    load_sem, side_send, side_recv, entered, far_send, far_recv, pair_send, pair_recv, sweep_send, sweep_recv,
):
    me = lax.axis_index("dom")

    def bit(p):
        return (me // (1 << p)) % 2

    member = (bit(5) + bit(6)) % 2 * 8 + (bit(3) + bit(4)) % 2 * 4 + (bit(1) + bit(2)) % 2 * 2 + bit(0)
    group = bit(6) * 4 + bit(4) * 2 + bit(2)
    group_low, group_high = bit(4) * 2 + bit(2), bit(6)

    def flipped(bits, k):
        other = me
        for n, p in enumerate(bits):
            if (k >> n) & 1:
                for q in p:
                    other = other + (1 - 2 * bit(q)) * (1 << q)
        return other

    def ring(low, high):
        at = bit(high) * 2 + bit(low)
        places = [(at + k) % 4 for k in range(4)]
        return [(v // 2) * (1 << high) + (v % 2) * (1 << low) for v in places]

    along_x, along_z, along_y = ring(1, 2), ring(3, 4), ring(5, 6)
    cores = [bit(0), 1 - bit(0)]
    steps = [(x, z, y) for x in range(4) for z in range(4) for y in range(4)]
    hops = (0, 1, 2, 1)
    steps = sorted(steps, key=lambda v: -(hops[v[0]] + hops[v[1]] + hops[v[2]]))
    all_peers = [along_x[x] + along_z[z] + along_y[y] + cores[0] for x, z, y in steps if (x, z, y) != (0, 0, 0)]
    my_high = member * 2 + bit(6)
    pair = ((my_high // 8) * 4 + group_low) * 8 + (my_high % 8 // 4) * 4 + bit(6) * 2
    my_slot = pair + bit(0)
    partner = along_x[0] + along_z[0] + along_y[0] + cores[1]
    cube_peers = [flipped(CUBE_BITS, k) for k in range(1, CUBE)]
    group_peers = [flipped(GROUP_BITS, k) for k in range(1, GROUPS)]
    left, right = (me + DEVICES - 1) % DEVICES, (me + 1) % DEVICES

    loads = []
    for n, (src, dst) in enumerate(
        (
            (b_h, b_v), (d_h, d_v), (agg_h, agg_v), (row_h, row_v), (cd_h, cd_v),
            (cq_h, cq_v), (ca_h, ca_v), (q_h, q_v), (a_h, a_v),
        )
    ):
        copy = pltpu.make_async_copy(src, dst, load_sem.at[n])
        copy.start()
        loads.append(copy)

    barrier = pltpu.get_barrier_semaphore()
    beside = [group_peers[k - 1] for k in (1, 2, 4)]
    for peer in cube_peers + beside + [left, right]:
        pl.semaphore_signal(barrier, inc=1, device_id=(peer,), device_id_type=MESH)

    def send(src, dst, send_sem, recv_sem, peer):
        pltpu.make_async_remote_copy(
            src_ref=src, dst_ref=dst, send_sem=send_sem, recv_sem=recv_sem,
            device_id=(peer,), device_id_type=MESH,
        ).start()

    def wait_bytes(ref, sem):
        pltpu.make_async_copy(ref, ref, sem).wait()

    lane = lax.broadcasted_iota(I32, (1, LANES), 1)

    def cols(n, count=1):
        return pl.ds(n * LANES, count * LANES)

    for n in range(4):
        loads[n].wait()
    place_row = position_of(row_v[...])
    stage[...] = jnp.zeros_like(stage)
    stage[pl.ds(3, 1), pl.ds(0, AGG_DEV)] = place_row.astype(F32)
    node_place = pick(stage[pl.ds(3, 1), :], agg_v[...])
    w0 = DAMP / d_v[...]
    f1[pl.ds(0, 3), :] = w0 * b_v[...]
    f1[pl.ds(4, 3), :] = w0
    for n in range(BLOCKS):
        f1[pl.ds(3, 1), cols(n)] = node_place[n : n + 1, :]
    pl.semaphore_wait(barrier, CUBE - 1 + 3 + 2)

    def to_right(n, src, dst):
        return pltpu.make_async_remote_copy(
            src_ref=src, dst_ref=dst, send_sem=side_send.at[n, 0], recv_sem=side_recv.at[n, 0],
            device_id=(right,), device_id_type=MESH,
        )

    def to_left(n, src, dst):
        return pltpu.make_async_remote_copy(
            src_ref=src, dst_ref=dst, send_sem=side_send.at[n, 1], recv_sem=side_recv.at[n, 1],
            device_id=(left,), device_id_type=MESH,
        )

    own_end, own_start = pl.ds(NODE_DEV, WIN), pl.ds(WIN, WIN)
    from_left, from_right = pl.ds(0, WIN), pl.ds(NODE_DEV + WIN, WIN)
    rightward = [
        to_right(0, f1.at[:, pl.ds(NODE_DEV - WIN, WIN)], f1l),
        to_right(1, f2.at[:, own_end], f2.at[:, from_left]),
        to_right(2, f4.at[:, own_end], f4.at[:, from_left]),
    ]
    leftward = [
        to_left(0, f1.at[:, pl.ds(0, WIN)], f1r),
        to_left(1, f2.at[:, own_start], f2.at[:, from_right]),
        to_left(2, f4.at[:, own_start], f4.at[:, from_right]),
    ]
    has_left, has_right = me > 0, me < DEVICES - 1

    def start_side(n, side):
        if side == "left":
            pl.when(has_left)(leftward[n].start)
        else:
            pl.when(has_right)(rightward[n].start)

    def await_side(n, side):
        if side == "left":
            pl.when(has_left)(rightward[n].wait_recv)
        else:
            pl.when(has_right)(leftward[n].wait_recv)

    def each_side(act, chip_first):
        @pl.when(bit(0) == 0)
        def _():
            for side in ("right", "left") if chip_first else ("left", "right"):
                act(side)

        @pl.when(bit(0) == 1)
        def _():
            for side in ("left", "right") if chip_first else ("right", "left"):
                act(side)

    start_side(0, "left")
    start_side(0, "right")

    def tell(n):
        pl.semaphore_signal(entered.at[n], inc=1, device_id=(beside[n],), device_id_type=MESH)

    tell(0)

    for n in range(4, 9):
        loads[n].wait()
    stage[pl.ds(0, 3), pl.ds(0, AGG_DEV)] = cd_v[...]
    own = stage[...]
    line = own[0:1]
    for n in range(1, 4):
        line = jnp.where(lane // AGG_DEV == n, pltpu.roll(own, 32 * n, 1)[n : n + 1], line)
    far0[my_slot] = line

    def send_group(n, ref):
        for peer in group_peers:
            send(ref.at[group], ref.at[group], far_send.at[n], far_recv.at[n], peer)

    def send_partner(n, ref):
        send(ref.at[my_slot], ref.at[my_slot], pair_send.at[n], pair_recv.at[n], partner)

    def send_all(n, ref):
        wait_bytes(ref.at[pl.ds(0, 1)], pair_recv.at[n])
        both = ref.at[pl.ds(pair, 2)]
        for peer in all_peers:
            send(both, both, far_send.at[n], far_recv.at[n], peer)

    def receive_all(n, ref, table):
        wait_bytes(ref.at[pl.ds(0, DEVICES - 2)], far_recv.at[n])
        order = [4 * (r // 4) + 2 * (r % 2) + r // 2 % 2 for r in range(8)]
        for t in range(4):
            parts = [jnp.concatenate([ref[32 * t + 8 * j + r] for r in order], axis=0) for j in range(4)]
            for c in range(table.shape[0]):
                whole = None
                for j in range(4):
                    moved = parts[j] if j == c else pltpu.roll(parts[j], 32 * ((j - c) % 4), 1)
                    whole = moved if j == 0 else jnp.where((lane // 32) == j, moved, whole)
                table[c, pl.ds(8 * t, 8), :] = whole

    def number_columns(n, carry):
        here = pl.ds(pl.multiple_of(n * LANES, LANES), LANES)
        q_s[pl.ds(24, 8), here] = jnp.zeros((8, LANES), I32)
        q_s[pl.ds(0, NNZ), here] = q_v[:, here] - (me * NODE_DEV - WIN + n * LANES)
        return carry

    def pack_one(e, carry):
        pack[e // 4, pl.ds(pl.multiple_of(32 * (e % 4), 32), 32), pl.ds(0, NNZ)] = ca_v[e // 3, e % 3]
        return carry

    send_partner(0, far0)
    pack[...] = jnp.zeros_like(pack)
    lax.fori_loop(0, 9, pack_one, 0)
    pack[2, pl.ds(32, 32), pl.ds(0, NNZ)] = position_of(cq_v[...]).astype(F32)
    for n in range(3):
        rm[group, pl.ds(32 * n, 32), :] = pack[n].T[0:32, :]

    lax.fori_loop(0, BLOCKS, number_columns, 0)

    def label_block(n, carry):
        label = lax.broadcasted_iota(I32, (LANES, LANES), 0) % AGG_DEV
        hit = agg_v[pl.ds(n, 1), :] == label
        onehot[:, pl.ds(pl.multiple_of(n * LANES, LANES), LANES)] = hit.astype(F32).astype(BF16)
        return carry

    lax.fori_loop(0, BLOCKS, label_block, 0)

    def couple_fine(blocks, field):
        for n in blocks:
            here = cols(n - SIDE)
            sums = [None] * 3
            for k in range(4):
                near = gather_rows(q_s[pl.ds(8 * k, 8), here], lambda r, c: field(c, n + r - SIDE), REACH)
                width = min(8, NNZ - 8 * k)
                for i in range(3):
                    term = None
                    for c in range(3):
                        part = a_v[i, c, pl.ds(8 * k, width), here] * near[c][:width]
                        term = part if term is None else term + part
                    term = jnp.sum(term, axis=0, keepdims=True) if width < 8 else term
                    if k == 0:
                        sums[i] = term
                    elif width == 8:
                        sums[i] = sums[i] + term
                    else:
                        sums[i] = jnp.sum(sums[i], axis=0, keepdims=True) + term
            for i in range(3):
                y_v[pl.ds(i, 1), here] = sums[i]

    def first_field(row, n, count=1):
        if n < SIDE:
            return f1l[row, cols(n, count)]
        if n < SIDE + BLOCKS:
            return f1[row, cols(n - SIDE, count)]
        return f1r[row, cols(n - SIDE - BLOCKS, count)]

    def start_field(c, n):
        return first_field(pl.ds(c, 1), n)

    middle = range(2 * SIDE, BLOCKS)
    border = {"left": range(SIDE, 2 * SIDE), "right": range(BLOCKS, BLOCKS + SIDE)}
    values, weights_at = pl.ds(0, 3), pl.ds(4, 3)

    pl.semaphore_wait(entered.at[0], 1)
    tell(1)
    couple_fine(middle, start_field)
    inside = cols(SIDE, BLOCKS)

    def second(blocks):
        here, count = cols(blocks[0] - SIDE, len(blocks)), len(blocks)
        f2[:, cols(blocks[0], count)] = (1.0 + KEEP) * f1[values, here] + f1[weights_at, here] * y_v[:, here]

    second(middle)
    pl.semaphore_wait(entered.at[1], 1)
    tell(2)

    def first_apply(side):
        await_side(0, side)
        couple_fine(border[side], start_field)
        second(border[side])
        start_side(1, side)

    each_side(first_apply, True)
    pl.semaphore_wait(entered.at[2], 1)
    send_all(0, far0)
    send_group(1, rm)
    couple_fine(middle, lambda c, n: f2[pl.ds(c, 1), cols(n)])

    r_v[...] = jnp.zeros_like(r_v)
    def second_apply(side):
        await_side(1, side)
        couple_fine(border[side], lambda c, n: f2[pl.ds(c, 1), cols(n)])

    each_side(second_apply, True)
    r_v[pl.ds(0, 3), :] = b_v[...] - d_v[...] * f2[:, inside] + y_v[...]
    rest = r_v[...]
    p0 = rest.astype(BF16).astype(F32)
    rest = rest - p0
    p1 = rest.astype(BF16).astype(F32)
    pieces = jnp.concatenate([p0, p1, rest - p1], axis=0).astype(BF16)
    sums = lax.dot_general(pieces, onehot[...], (((1,), (1,)), ((), ())), preferred_element_type=F32)
    sums = sums[0:4] + sums[8:12] + sums[16:20]
    line = sums[0:1]
    for n in range(1, 3):
        line = jnp.where(lane // AGG_DEV == n, sums[n : n + 1], line)
    far1[my_slot] = line
    send_partner(2, far1)
    send_all(2, far1)

    receive_all(0, far0, tab0)
    inverse = None
    for r in range(CROWS):
        place = tab0[3, pl.ds(r, 1), :].astype(I32)
        high, low = place >> 7, place & 127
        at_high = lax.broadcasted_iota(I32, (CROWS, LANES), 0) == high
        at_low = (lax.broadcasted_iota(I32, (LANES, LANES), 0) == low).astype(F32).astype(BF16)
        weights = jnp.concatenate(
            [
                jnp.where(at_high, jnp.float32(r), 0.0),
                jnp.where(at_high, lane.astype(F32), 0.0),
            ],
            axis=0,
        ).astype(BF16)
        term = lax.dot_general(weights, at_low, (((1,), (1,)), ((), ())), preferred_element_type=F32)
        inverse = term if inverse is None else inverse + term
    inv_v[...] = (inverse[0:CROWS] * LANES + inverse[CROWS : 2 * CROWS]).astype(I32)
    for c in range(3):
        tab0[c] = DAMP / tab0[c]
    for r in range(CROWS):
        for c in range(3):
            wbuf[r // 2, pl.ds(4 * (r % 2) + c, 1), :] = tab0[c, pl.ds(r, 1), :]
    wait_bytes(rm.at[pl.ds(0, GROUPS - 1)], far_recv.at[1])
    spare = {}
    for h in range(2):
        for e4 in range(3):
            for k in range(4):
                parts = [rm[4 * h + j, pl.ds(32 * e4 + 8 * k, 8), :] for j in range(4)]
                for s in range(4):
                    e = 4 * e4 + s
                    if e > 9:
                        continue
                    whole = None
                    for j in range(4):
                        moved = parts[j] if j == s else pltpu.roll(parts[j], 32 * ((j - s) % 4), 1)
                        whole = moved if j == 0 else jnp.where((lane // 32) == j, moved, whole)
                    rows, lines = pl.ds(8 * k, 8), pl.ds(LANES * h, LANES)
                    if k == 3:
                        lines = pl.ds(0, LANES)
                        if h == 0:
                            spare[e] = whole
                            continue
                        whole = spare[e] + pltpu.roll(whole, NNZ - 24, 0)
                    if e < 9:
                        mx[e, rows, lines] = whole
                    else:
                        mp[rows, lines] = whole.astype(I32)

    idx_v[...] = jnp.zeros_like(idx_v)
    for n in range(WIDE):
        idx_v[pl.ds(n, 1), :] = first_field(pl.ds(3, 1), n).astype(I32)

    receive_all(2, far1, tab1)

    for t in range(CROWS // 8):
        sums = gather_rows(inv_v[pl.ds(8 * t, 8), :], lambda r, c: tab1[c, pl.ds(r, 1), :], CROWS)
        for c in range(3):
            value = sums[c] * tab0[c, pl.ds(8 * t, 8), :]
            for n in range(8):
                r = 8 * t + n
                cbuf[0, r // 2, pl.ds(4 * (r % 2) + c, 1), :] = value[n : n + 1, :]

    unused = lax.broadcasted_iota(I32, (8, LANES), 0) % 4 == 3
    first = jnp.where(unused, 0.0, cbuf[0, member])
    weight = jnp.where(unused, 0.0, wbuf[member])

    def place(k):
        slot = member
        for p, w in enumerate((1, 2, 4, 8)):
            if (k >> p) & 1:
                slot = slot + (1 - 2 * ((member // w) % 2)) * w
        return slot

    stages = [[k for k in range(CUBE) if bin(k >> 1).count("1") == hops] for hops in range(4)]

    def coarse_values(n, places, arrive):
        found = [[jnp.zeros((8, LANES), F32)] * 3 for _ in places]
        for stage_of in stages:
            for k in stage_of:
                if k and arrive:
                    there = cbuf.at[n, place(k)]
                    pltpu.make_async_copy(there, there, sweep_recv.at[n - 1, k]).wait()
            for t, where in enumerate(places):
                high, low = where() >> 7, where() & 127
                for k in stage_of:
                    slot = place(k)
                    for h in range(2):
                        hit = high == slot * 2 + h
                        for c in range(3):
                            taken = pick(cbuf[n, slot, pl.ds(4 * h + c, 1), :], low)
                            found[t][c] = jnp.where(hit, taken, found[t][c])
        return found

    tiles = [(pl.ds(8 * k, 8), pl.ds(LANES * h, LANES)) for h in range(2) for k in range(3)]
    tiles.append((pl.ds(24, 8), pl.ds(0, LANES)))
    sublane = lax.broadcasted_iota(I32, (8, LANES), 0)

    def sweep(n, current, arrive):
        near = coarse_values(n, [lambda at=at: mp[at] for at in tiles], arrive)

        def product(i, which):
            total = None
            for t in which:
                for c in range(3):
                    part = mx[3 * i + c, tiles[t][0], tiles[t][1]] * near[t][c]
                    total = part if total is None else total + part
            return total

        shared = [product(i, (6,)) for i in range(3)]
        totals = []
        for h in range(2):
            for i in range(3):
                mine = sublane < NNZ - 24 if h == 0 else sublane >= NNZ - 24
                total = product(i, range(3 * h, 3 * h + 3)) + jnp.where(mine, shared[i], 0.0)
                totals.append(jnp.sum(total, axis=0, keepdims=True))
            totals.append(jnp.zeros((1, LANES), F32))
        current = KEEP * current + first + weight * jnp.concatenate(totals, axis=0)
        cbuf[n + 1, member] = current
        mine = cbuf.at[n + 1, member]
        for k in reversed(range(1, CUBE)):
            send(mine, mine, sweep_send.at[n], sweep_recv.at[n, k], cube_peers[k - 1])
        return current

    last = lax.fori_loop(1, CSWEEPS - 1, lambda n, current: sweep(n, current, True), sweep(0, first, False))

    found = coarse_values(CSWEEPS - 1, [lambda t=t: idx_v[pl.ds(8 * t, 8), :] for t in range(2)], True)
    for n in range(WIDE):
        for c in range(3):
            f3[pl.ds(c, 1), cols(n)] = f2[pl.ds(c, 1), cols(n)] + found[n // 8][c][n % 8 : n % 8 + 1, :]

    def smooth(old, n, count):
        here = cols(n - SIDE, count)
        return KEEP * old[:, cols(n, count)] + f1[values, here] + f1[weights_at, here] * y_v[:, here]

    def third_apply(side):
        couple_fine(border[side], lambda c, n: f3[pl.ds(c, 1), cols(n)])
        f4[:, cols(border[side][0], SIDE)] = smooth(f3, border[side][0], SIDE)
        start_side(2, side)

    each_side(third_apply, False)
    couple_fine(middle, lambda c, n: f3[pl.ds(c, 1), cols(n)])
    f4[:, cols(2 * SIDE, BLOCKS - 2 * SIDE)] = smooth(f3, 2 * SIDE, BLOCKS - 2 * SIDE)
    couple_fine(middle, lambda c, n: f4[pl.ds(c, 1), cols(n)])

    part = jnp.where(group_high == 0, last[0:4], last[4:8])
    moved = part
    for k in range(1, 4):
        moved = jnp.where(group_low == k, pltpu.roll(part, LANES - 32 * k, 1), moved)
    out_o[:, pl.ds(NODE_DEV, LANES)] = moved[0:3]

    def last_apply(side):
        await_side(2, side)
        couple_fine(border[side], lambda c, n: f4[pl.ds(c, 1), cols(n)])

    each_side(last_apply, True)
    out_o[:, pl.ds(0, NODE_DEV)] = smooth(f4, SIDE, BLOCKS)

    for n in range(3):
        pl.when(has_right)(rightward[n].wait_send)
        pl.when(has_left)(leftward[n].wait_send)
    for n, (ref, count) in enumerate(((far0, DEVICES - 1), (rm, GROUPS), (far1, DEVICES - 1))):
        wait_bytes(ref.at[pl.ds(0, count - 1)], far_send.at[n])
        if n != 1:
            wait_bytes(ref.at[pl.ds(0, 1)], pair_send.at[n])
    for n in range(CSWEEPS - 1):
        wait_bytes(cbuf.at[n + 1, pl.ds(0, CUBE - 1)], sweep_send.at[n])


def split(all_ref, sol_o, cor_o):
    sol_o[...] = all_ref[:, pl.ds(0, NODE_DEV)]
    cor_o[...] = all_ref[:, pl.ds(NODE_DEV, LANES)][:, 0:AGG_DEV]


def body(b, d, q, a, agg, row, cd, cq, ca):
    any_spec = pl.BlockSpec(memory_space=pl.ANY)
    vmem = pl.BlockSpec(memory_space=pltpu.VMEM)
    dma = pltpu.SemaphoreType.DMA
    out = pl.pallas_call(
        kernel,
        out_shape=pltpu.VMEM((3, NODE_DEV + LANES), F32),
        in_specs=[any_spec] * 9,
        out_specs=vmem,
        scratch_shapes=[
            pltpu.VMEM((3, NODE_DEV), F32),
            pltpu.VMEM((3, NODE_DEV), F32),
            pltpu.VMEM((NNZ, NODE_DEV), I32),
            pltpu.VMEM((3, 3, NNZ, NODE_DEV), F32),
            pltpu.VMEM((BLOCKS, LANES), I32),
            pltpu.VMEM((1, AGG_DEV), I32),
            pltpu.VMEM((3, AGG_DEV), F32),
            pltpu.VMEM((AGG_DEV, NNZ), I32),
            pltpu.VMEM((3, 3, AGG_DEV, NNZ), F32),
            pltpu.VMEM((32, NODE_DEV), I32),
            pltpu.VMEM((3, NODE_DEV), F32),
            pltpu.VMEM((8, NODE_DEV), F32),
            pltpu.VMEM((LANES, NODE_DEV), BF16),
            pltpu.VMEM((16, LANES), I32),
            pltpu.VMEM((8, NODE_DEV), F32),
            pltpu.VMEM((8, WIN), F32),
            pltpu.VMEM((8, WIN), F32),
            pltpu.VMEM((3, WIDE * LANES), F32),
            pltpu.VMEM((3, WIDE * LANES), F32),
            pltpu.VMEM((3, WIDE * LANES), F32),
            pltpu.VMEM((4, LANES), F32),
            pltpu.VMEM((DEVICES, 1, LANES), F32),
            pltpu.VMEM((DEVICES, 1, LANES), F32),
            pltpu.VMEM((4, CROWS, LANES), F32),
            pltpu.VMEM((3, CROWS, LANES), F32),
            pltpu.VMEM((3, LANES, LANES), F32),
            pltpu.VMEM((GROUPS, 96, LANES), F32),
            pltpu.VMEM((9, 32, 2 * LANES), F32),
            pltpu.VMEM((32, 2 * LANES), I32),
            pltpu.VMEM((CROWS, LANES), I32),
            pltpu.VMEM((CUBE, 8, LANES), F32),
            pltpu.VMEM((CSWEEPS, CUBE, 8, LANES), F32),
            dma((9,)),
            dma((3, 2)),
            dma((3, 2)),
            pltpu.SemaphoreType.REGULAR((3,)),
            dma((3,)),
            dma((3,)),
            dma((3,)),
            dma((3,)),
            dma((CSWEEPS - 1,)),
            dma((CSWEEPS - 1, CUBE)),
        ],
        compiler_params=pltpu.CompilerParams(collective_id=0, has_side_effects=True),
        name="vcycle",
    )(
        b.T,
        d.T,
        q.T,
        a.transpose(2, 3, 1, 0),
        agg.reshape(BLOCKS, LANES),
        row.reshape(1, AGG_DEV),
        cd.T,
        cq,
        ca.transpose(2, 3, 0, 1),
    )
    sol, cor = pl.pallas_call(
        split,
        out_shape=(
            jax.ShapeDtypeStruct((3, NODE_DEV), F32),
            jax.ShapeDtypeStruct((3, AGG_DEV), F32),
        ),
        in_specs=[vmem],
        out_specs=(vmem, vmem),
        name="split",
    )(pltpu.with_memory_space_constraint(out, pltpu.VMEM))
    return sol.T, cor.T


def solution(mesh):
    rows, line = P("dom", None), P("dom")
    blocks = P("dom", None, None, None)
    return jax.shard_map(
        body,
        mesh=mesh,
        in_specs=(rows, rows, rows, blocks, line, line, rows, rows, blocks),
        out_specs=(rows, rows),
        check_vma=False,
    )
```

```python
import jax
import jax.numpy as jnp
from jax import lax
from jax.experimental import pallas as pl
from jax.experimental.pallas import tpu as pltpu
from jax.sharding import PartitionSpec as P

DEVICES = 128
NODE_DEV = 1024
WIN = 256
NNZ = 27
AGG_DEV = 32
CSWEEPS = 6
LANES = 128
BLOCKS = NODE_DEV // LANES
SIDE = WIN // LANES
WIDE = BLOCKS + 2 * SIDE
REACH = 2 * SIDE + 1
CUBE = 16
GROUPS = 8
CROWS = 32
DAMP = 0.7
KEEP = 1.0 - DAMP
CUBE_BITS = ((0,), (1,), (3,), (5,))
GROUP_BITS = ((1, 2), (3, 4), (5, 6))
MESH = pl.DeviceIdType.MESH
F32, I32, BF16 = jnp.float32, jnp.int32, jnp.bfloat16


def position_of(row):
    def bit(p):
        return (row >> p) & 1

    high = (bit(10) ^ bit(11)) * 16 + (bit(8) ^ bit(9)) * 8 + (bit(6) ^ bit(7)) * 4 + bit(5) * 2 + bit(11)
    lane = bit(9) * 64 + bit(7) * 32 + (row & 31)
    return high * LANES + lane


def spread(row):
    return jnp.broadcast_to(row, (8, LANES))


def pick(row, lane):
    return jnp.take_along_axis(spread(row), lane, axis=1, mode="promise_in_bounds")


def gather_rows(place, rows, count):
    high, lane = place >> 7, place & 127
    values = [None] * 3
    for r in range(count):
        hit = high == r
        for c in range(3):
            taken = pick(rows(r, c), lane)
            values[c] = taken if r == 0 else jnp.where(hit, taken, values[c])
    return values


def kernel(
    b_h, d_h, q_h, a_h, agg_h, row_h, cd_h, cq_h, ca_h,
    out_o,
    b_v, d_v, q_v, a_v, agg_v, row_v, cd_v, cq_v, ca_v,
 q_s, y_v, r_v, onehot, idx_v,
    f1, f1l, f1r, f2, f3, f4,
    stage, far0, far1, tab0, tab1,
    pack, rm, mx, mp,
    inv_v, wbuf, cbuf,
    load_sem, side_send, side_recv, entered, far_send, far_recv, pair_send, pair_recv, sweep_send, sweep_recv,
):
    me = lax.axis_index("dom")

    def bit(p):
        return (me // (1 << p)) % 2

    member = (bit(5) + bit(6)) % 2 * 8 + (bit(3) + bit(4)) % 2 * 4 + (bit(1) + bit(2)) % 2 * 2 + bit(0)
    group = bit(6) * 4 + bit(4) * 2 + bit(2)
    group_low, group_high = bit(4) * 2 + bit(2), bit(6)

    def flipped(bits, k):
        other = me
        for n, p in enumerate(bits):
            if (k >> n) & 1:
                for q in p:
                    other = other + (1 - 2 * bit(q)) * (1 << q)
        return other

    def ring(low, high):
        at = bit(high) * 2 + bit(low)
        places = [(at + k) % 4 for k in range(4)]
        return [(v // 2) * (1 << high) + (v % 2) * (1 << low) for v in places]

    along_x, along_z, along_y = ring(1, 2), ring(3, 4), ring(5, 6)
    cores = [bit(0), 1 - bit(0)]
    steps = [(x, z, y) for x in range(4) for z in range(4) for y in range(4)]
    hops = (0, 1, 2, 1)
    steps = sorted(steps, key=lambda v: -(hops[v[0]] + hops[v[1]] + hops[v[2]]))
    all_peers = [along_x[x] + along_z[z] + along_y[y] + cores[0] for x, z, y in steps if (x, z, y) != (0, 0, 0)]
    my_high = member * 2 + bit(6)
    pair = ((my_high // 8) * 4 + group_low) * 8 + (my_high % 8 // 4) * 4 + bit(6) * 2
    my_slot = pair + bit(0)
    partner = along_x[0] + along_z[0] + along_y[0] + cores[1]
    cube_peers = [flipped(CUBE_BITS, k) for k in range(1, CUBE)]
    group_peers = [flipped(GROUP_BITS, k) for k in range(1, GROUPS)]
    left, right = (me + DEVICES - 1) % DEVICES, (me + 1) % DEVICES

    loads = []
    for n, (src, dst) in enumerate(
        (
            (b_h, b_v), (d_h, d_v), (agg_h, agg_v), (row_h, row_v), (cd_h, cd_v),
            (cq_h, cq_v), (ca_h, ca_v), (q_h, q_v), (a_h, a_v),
        )
    ):
        copy = pltpu.make_async_copy(src, dst, load_sem.at[n])
        copy.start()
        loads.append(copy)

    barrier = pltpu.get_barrier_semaphore()
    beside = [group_peers[k - 1] for k in (1, 2, 4)]
    for peer in cube_peers + beside + [left, right]:
        pl.semaphore_signal(barrier, inc=1, device_id=(peer,), device_id_type=MESH)

    def send(src, dst, send_sem, recv_sem, peer):
        pltpu.make_async_remote_copy(
            src_ref=src, dst_ref=dst, send_sem=send_sem, recv_sem=recv_sem,
            device_id=(peer,), device_id_type=MESH,
        ).start()

    def wait_bytes(ref, sem):
        pltpu.make_async_copy(ref, ref, sem).wait()

    lane = lax.broadcasted_iota(I32, (1, LANES), 1)

    def cols(n, count=1):
        return pl.ds(n * LANES, count * LANES)

    for n in range(4):
        loads[n].wait()
    place_row = position_of(row_v[...])
    stage[...] = jnp.zeros_like(stage)
    stage[pl.ds(3, 1), pl.ds(0, AGG_DEV)] = place_row.astype(F32)
    node_place = pick(stage[pl.ds(3, 1), :], agg_v[...])
    w0 = DAMP / d_v[...]
    f1[pl.ds(0, 3), :] = w0 * b_v[...]
    f1[pl.ds(4, 3), :] = w0
    for n in range(BLOCKS):
        f1[pl.ds(3, 1), cols(n)] = node_place[n : n + 1, :]
    pl.semaphore_wait(barrier, CUBE - 1 + 3 + 2)

    def to_right(n, src, dst):
        return pltpu.make_async_remote_copy(
            src_ref=src, dst_ref=dst, send_sem=side_send.at[n, 0], recv_sem=side_recv.at[n, 0],
            device_id=(right,), device_id_type=MESH,
        )

    def to_left(n, src, dst):
        return pltpu.make_async_remote_copy(
            src_ref=src, dst_ref=dst, send_sem=side_send.at[n, 1], recv_sem=side_recv.at[n, 1],
            device_id=(left,), device_id_type=MESH,
        )

    own_end, own_start = pl.ds(NODE_DEV, WIN), pl.ds(WIN, WIN)
    from_left, from_right = pl.ds(0, WIN), pl.ds(NODE_DEV + WIN, WIN)
    rightward = [
        to_right(0, f1.at[:, pl.ds(NODE_DEV - WIN, WIN)], f1l),
        to_right(1, f2.at[:, own_end], f2.at[:, from_left]),
        to_right(2, f4.at[:, own_end], f4.at[:, from_left]),
    ]
    leftward = [
        to_left(0, f1.at[:, pl.ds(0, WIN)], f1r),
        to_left(1, f2.at[:, own_start], f2.at[:, from_right]),
        to_left(2, f4.at[:, own_start], f4.at[:, from_right]),
    ]
    has_left, has_right = me > 0, me < DEVICES - 1

    def start_side(n, side):
        if side == "left":
            pl.when(has_left)(leftward[n].start)
        else:
            pl.when(has_right)(rightward[n].start)

    def await_side(n, side):
        if side == "left":
            pl.when(has_left)(rightward[n].wait_recv)
        else:
            pl.when(has_right)(leftward[n].wait_recv)

    def each_side(act, chip_first):
        @pl.when(bit(0) == 0)
        def _():
            for side in ("right", "left") if chip_first else ("left", "right"):
                act(side)

        @pl.when(bit(0) == 1)
        def _():
            for side in ("left", "right") if chip_first else ("right", "left"):
                act(side)

    start_side(0, "left")
    start_side(0, "right")

    def tell(n):
        pl.semaphore_signal(entered.at[n], inc=1, device_id=(beside[n],), device_id_type=MESH)

    tell(0)

    for n in range(4, 9):
        loads[n].wait()
    stage[pl.ds(0, 3), pl.ds(0, AGG_DEV)] = cd_v[...]
    own = stage[...]
    line = own[0:1]
    for n in range(1, 4):
        line = jnp.where(lane // AGG_DEV == n, pltpu.roll(own, 32 * n, 1)[n : n + 1], line)
    far0[my_slot] = line

    def send_group(n, ref):
        for peer in group_peers:
            send(ref.at[group], ref.at[group], far_send.at[n], far_recv.at[n], peer)

    def send_partner(n, ref):
        send(ref.at[my_slot], ref.at[my_slot], pair_send.at[n], pair_recv.at[n], partner)

    def send_all(n, ref):
        wait_bytes(ref.at[pl.ds(0, 1)], pair_recv.at[n])
        both = ref.at[pl.ds(pair, 2)]
        for peer in all_peers:
            send(both, both, far_send.at[n], far_recv.at[n], peer)

    def receive_all(n, ref, table):
        wait_bytes(ref.at[pl.ds(0, DEVICES - 2)], far_recv.at[n])
        order = [4 * (r // 4) + 2 * (r % 2) + r // 2 % 2 for r in range(8)]
        for t in range(4):
            parts = [jnp.concatenate([ref[32 * t + 8 * j + r] for r in order], axis=0) for j in range(4)]
            for c in range(table.shape[0]):
                whole = None
                for j in range(4):
                    moved = parts[j] if j == c else pltpu.roll(parts[j], 32 * ((j - c) % 4), 1)
                    whole = moved if j == 0 else jnp.where((lane // 32) == j, moved, whole)
                table[c, pl.ds(8 * t, 8), :] = whole

    def number_columns(n, carry):
        here = pl.ds(pl.multiple_of(n * LANES, LANES), LANES)
        q_s[pl.ds(24, 8), here] = jnp.zeros((8, LANES), I32)
        q_s[pl.ds(0, NNZ), here] = q_v[:, here] - (me * NODE_DEV - WIN + n * LANES)
        return carry

    def pack_one(e, carry):
        pack[e // 4, pl.ds(pl.multiple_of(32 * (e % 4), 32), 32), pl.ds(0, NNZ)] = ca_v[e // 3, e % 3]
        return carry

    send_partner(0, far0)
    pack[...] = jnp.zeros_like(pack)
    lax.fori_loop(0, 9, pack_one, 0)
    pack[2, pl.ds(32, 32), pl.ds(0, NNZ)] = position_of(cq_v[...]).astype(F32)
    for n in range(3):
        rm[group, pl.ds(32 * n, 32), :] = pack[n].T[0:32, :]

    lax.fori_loop(0, BLOCKS, number_columns, 0)

    def label_block(n, carry):
        label = lax.broadcasted_iota(I32, (LANES, LANES), 0) % AGG_DEV
        hit = agg_v[pl.ds(n, 1), :] == label
        onehot[:, pl.ds(pl.multiple_of(n * LANES, LANES), LANES)] = hit.astype(F32).astype(BF16)
        return carry

    lax.fori_loop(0, BLOCKS, label_block, 0)

    def couple_fine(blocks, field):
        for n in blocks:
            here = cols(n - SIDE)
            sums = [None] * 3
            for k in range(4):
                near = gather_rows(q_s[pl.ds(8 * k, 8), here], lambda r, c: field(c, n + r - SIDE), REACH)
                width = min(8, NNZ - 8 * k)
                for i in range(3):
                    term = None
                    for c in range(3):
                        part = a_v[i, c, pl.ds(8 * k, width), here] * near[c][:width]
                        term = part if term is None else term + part
                    term = jnp.sum(term, axis=0, keepdims=True) if width < 8 else term
                    if k == 0:
                        sums[i] = term
                    elif width == 8:
                        sums[i] = sums[i] + term
                    else:
                        sums[i] = jnp.sum(sums[i], axis=0, keepdims=True) + term
            for i in range(3):
                y_v[pl.ds(i, 1), here] = sums[i]

    def first_field(row, n, count=1):
        if n < SIDE:
            return f1l[row, cols(n, count)]
        if n < SIDE + BLOCKS:
            return f1[row, cols(n - SIDE, count)]
        return f1r[row, cols(n - SIDE - BLOCKS, count)]

    def start_field(c, n):
        return first_field(pl.ds(c, 1), n)

    middle = range(2 * SIDE, BLOCKS)
    border = {"left": range(SIDE, 2 * SIDE), "right": range(BLOCKS, BLOCKS + SIDE)}
    values, weights_at = pl.ds(0, 3), pl.ds(4, 3)

    pl.semaphore_wait(entered.at[0], 1)
    tell(1)
    couple_fine(middle, start_field)
    inside = cols(SIDE, BLOCKS)

    def second(blocks):
        here, count = cols(blocks[0] - SIDE, len(blocks)), len(blocks)
        f2[:, cols(blocks[0], count)] = (1.0 + KEEP) * f1[values, here] + f1[weights_at, here] * y_v[:, here]

    second(middle)
    pl.semaphore_wait(entered.at[1], 1)
    tell(2)

    def first_apply(side):
        await_side(0, side)
        couple_fine(border[side], start_field)
        second(border[side])
        start_side(1, side)

    each_side(first_apply, True)
    couple_fine(middle, lambda c, n: f2[pl.ds(c, 1), cols(n)])
    pl.semaphore_wait(entered.at[2], 1)
    send_all(0, far0)
    send_group(1, rm)

    r_v[...] = jnp.zeros_like(r_v)
    def second_apply(side):
        await_side(1, side)
        couple_fine(border[side], lambda c, n: f2[pl.ds(c, 1), cols(n)])

    each_side(second_apply, True)
    r_v[pl.ds(0, 3), :] = b_v[...] - d_v[...] * f2[:, inside] + y_v[...]
    rest = r_v[...]
    p0 = rest.astype(BF16).astype(F32)
    rest = rest - p0
    p1 = rest.astype(BF16).astype(F32)
    pieces = jnp.concatenate([p0, p1, rest - p1], axis=0).astype(BF16)
    sums = lax.dot_general(pieces, onehot[...], (((1,), (1,)), ((), ())), preferred_element_type=F32)
    sums = sums[0:4] + sums[8:12] + sums[16:20]
    line = sums[0:1]
    for n in range(1, 3):
        line = jnp.where(lane // AGG_DEV == n, sums[n : n + 1], line)
    far1[my_slot] = line
    send_partner(2, far1)
    send_all(2, far1)

    receive_all(0, far0, tab0)
    inverse = None
    for r in range(CROWS):
        place = tab0[3, pl.ds(r, 1), :].astype(I32)
        high, low = place >> 7, place & 127
        at_high = lax.broadcasted_iota(I32, (CROWS, LANES), 0) == high
        at_low = (lax.broadcasted_iota(I32, (LANES, LANES), 0) == low).astype(F32).astype(BF16)
        weights = jnp.concatenate(
            [
                jnp.where(at_high, jnp.float32(r), 0.0),
                jnp.where(at_high, lane.astype(F32), 0.0),
            ],
            axis=0,
        ).astype(BF16)
        term = lax.dot_general(weights, at_low, (((1,), (1,)), ((), ())), preferred_element_type=F32)
        inverse = term if inverse is None else inverse + term
    inv_v[...] = (inverse[0:CROWS] * LANES + inverse[CROWS : 2 * CROWS]).astype(I32)
    for c in range(3):
        tab0[c] = DAMP / tab0[c]
    for r in range(CROWS):
        for c in range(3):
            wbuf[r // 2, pl.ds(4 * (r % 2) + c, 1), :] = tab0[c, pl.ds(r, 1), :]
    wait_bytes(rm.at[pl.ds(0, GROUPS - 1)], far_recv.at[1])
    spare = {}
    for h in range(2):
        for e4 in range(3):
            for k in range(4):
                parts = [rm[4 * h + j, pl.ds(32 * e4 + 8 * k, 8), :] for j in range(4)]
                for s in range(4):
                    e = 4 * e4 + s
                    if e > 9:
                        continue
                    whole = None
                    for j in range(4):
                        moved = parts[j] if j == s else pltpu.roll(parts[j], 32 * ((j - s) % 4), 1)
                        whole = moved if j == 0 else jnp.where((lane // 32) == j, moved, whole)
                    rows, lines = pl.ds(8 * k, 8), pl.ds(LANES * h, LANES)
                    if k == 3:
                        lines = pl.ds(0, LANES)
                        if h == 0:
                            spare[e] = whole
                            continue
                        whole = spare[e] + pltpu.roll(whole, NNZ - 24, 0)
                    if e < 9:
                        mx[e, rows, lines] = whole
                    else:
                        mp[rows, lines] = whole.astype(I32)

    idx_v[...] = jnp.zeros_like(idx_v)
    for n in range(WIDE):
        idx_v[pl.ds(n, 1), :] = first_field(pl.ds(3, 1), n).astype(I32)

    receive_all(2, far1, tab1)

    for t in range(CROWS // 8):
        sums = gather_rows(inv_v[pl.ds(8 * t, 8), :], lambda r, c: tab1[c, pl.ds(r, 1), :], CROWS)
        for c in range(3):
            value = sums[c] * tab0[c, pl.ds(8 * t, 8), :]
            for n in range(8):
                r = 8 * t + n
                cbuf[0, r // 2, pl.ds(4 * (r % 2) + c, 1), :] = value[n : n + 1, :]

    unused = lax.broadcasted_iota(I32, (8, LANES), 0) % 4 == 3
    first = jnp.where(unused, 0.0, cbuf[0, member])
    weight = jnp.where(unused, 0.0, wbuf[member])

    def place(k):
        slot = member
        for p, w in enumerate((1, 2, 4, 8)):
            if (k >> p) & 1:
                slot = slot + (1 - 2 * ((member // w) % 2)) * w
        return slot

    stages = [[k for k in range(CUBE) if bin(k >> 1).count("1") == hops] for hops in range(4)]

    def coarse_values(n, places, arrive):
        found = [[jnp.zeros((8, LANES), F32)] * 3 for _ in places]
        for stage_of in stages:
            for k in stage_of:
                if k and arrive:
                    there = cbuf.at[n, place(k)]
                    pltpu.make_async_copy(there, there, sweep_recv.at[n - 1, k]).wait()
            for t, where in enumerate(places):
                high, low = where() >> 7, where() & 127
                for k in stage_of:
                    slot = place(k)
                    for h in range(2):
                        hit = high == slot * 2 + h
                        for c in range(3):
                            taken = pick(cbuf[n, slot, pl.ds(4 * h + c, 1), :], low)
                            found[t][c] = jnp.where(hit, taken, found[t][c])
        return found

    tiles = [(pl.ds(8 * k, 8), pl.ds(LANES * h, LANES)) for h in range(2) for k in range(3)]
    tiles.append((pl.ds(24, 8), pl.ds(0, LANES)))
    sublane = lax.broadcasted_iota(I32, (8, LANES), 0)

    def sweep(n, current, arrive):
        near = coarse_values(n, [lambda at=at: mp[at] for at in tiles], arrive)

        def product(i, which):
            total = None
            for t in which:
                for c in range(3):
                    part = mx[3 * i + c, tiles[t][0], tiles[t][1]] * near[t][c]
                    total = part if total is None else total + part
            return total

        shared = [product(i, (6,)) for i in range(3)]
        totals = []
        for h in range(2):
            for i in range(3):
                mine = sublane < NNZ - 24 if h == 0 else sublane >= NNZ - 24
                total = product(i, range(3 * h, 3 * h + 3)) + jnp.where(mine, shared[i], 0.0)
                totals.append(jnp.sum(total, axis=0, keepdims=True))
            totals.append(jnp.zeros((1, LANES), F32))
        current = KEEP * current + first + weight * jnp.concatenate(totals, axis=0)
        cbuf[n + 1, member] = current
        mine = cbuf.at[n + 1, member]
        for k in reversed(range(1, CUBE)):
            send(mine, mine, sweep_send.at[n], sweep_recv.at[n, k], cube_peers[k - 1])
        return current

    last = lax.fori_loop(1, CSWEEPS - 1, lambda n, current: sweep(n, current, True), sweep(0, first, False))

    found = coarse_values(CSWEEPS - 1, [lambda t=t: idx_v[pl.ds(8 * t, 8), :] for t in range(2)], True)
    for n in range(WIDE):
        for c in range(3):
            f3[pl.ds(c, 1), cols(n)] = f2[pl.ds(c, 1), cols(n)] + found[n // 8][c][n % 8 : n % 8 + 1, :]

    def smooth(old, n, count):
        here = cols(n - SIDE, count)
        return KEEP * old[:, cols(n, count)] + f1[values, here] + f1[weights_at, here] * y_v[:, here]

    def third_apply(side):
        couple_fine(border[side], lambda c, n: f3[pl.ds(c, 1), cols(n)])
        f4[:, cols(border[side][0], SIDE)] = smooth(f3, border[side][0], SIDE)
        start_side(2, side)

    each_side(third_apply, False)
    couple_fine(middle, lambda c, n: f3[pl.ds(c, 1), cols(n)])
    f4[:, cols(2 * SIDE, BLOCKS - 2 * SIDE)] = smooth(f3, 2 * SIDE, BLOCKS - 2 * SIDE)
    couple_fine(middle, lambda c, n: f4[pl.ds(c, 1), cols(n)])

    part = jnp.where(group_high == 0, last[0:4], last[4:8])
    moved = part
    for k in range(1, 4):
        moved = jnp.where(group_low == k, pltpu.roll(part, LANES - 32 * k, 1), moved)
    out_o[:, pl.ds(NODE_DEV, LANES)] = moved[0:3]

    def last_apply(side):
        await_side(2, side)
        couple_fine(border[side], lambda c, n: f4[pl.ds(c, 1), cols(n)])

    each_side(last_apply, True)
    out_o[:, pl.ds(0, NODE_DEV)] = smooth(f4, SIDE, BLOCKS)

    for n in range(3):
        pl.when(has_right)(rightward[n].wait_send)
        pl.when(has_left)(leftward[n].wait_send)
    for n, (ref, count) in enumerate(((far0, DEVICES - 1), (rm, GROUPS), (far1, DEVICES - 1))):
        wait_bytes(ref.at[pl.ds(0, count - 1)], far_send.at[n])
        if n != 1:
            wait_bytes(ref.at[pl.ds(0, 1)], pair_send.at[n])
    for n in range(CSWEEPS - 1):
        wait_bytes(cbuf.at[n + 1, pl.ds(0, CUBE - 1)], sweep_send.at[n])


def split(all_ref, sol_o, cor_o):
    sol_o[...] = all_ref[:, pl.ds(0, NODE_DEV)]
    cor_o[...] = all_ref[:, pl.ds(NODE_DEV, LANES)][:, 0:AGG_DEV]


def body(b, d, q, a, agg, row, cd, cq, ca):
    any_spec = pl.BlockSpec(memory_space=pl.ANY)
    vmem = pl.BlockSpec(memory_space=pltpu.VMEM)
    dma = pltpu.SemaphoreType.DMA
    out = pl.pallas_call(
        kernel,
        out_shape=pltpu.VMEM((3, NODE_DEV + LANES), F32),
        in_specs=[any_spec] * 9,
        out_specs=vmem,
        scratch_shapes=[
            pltpu.VMEM((3, NODE_DEV), F32),
            pltpu.VMEM((3, NODE_DEV), F32),
            pltpu.VMEM((NNZ, NODE_DEV), I32),
            pltpu.VMEM((3, 3, NNZ, NODE_DEV), F32),
            pltpu.VMEM((BLOCKS, LANES), I32),
            pltpu.VMEM((1, AGG_DEV), I32),
            pltpu.VMEM((3, AGG_DEV), F32),
            pltpu.VMEM((AGG_DEV, NNZ), I32),
            pltpu.VMEM((3, 3, AGG_DEV, NNZ), F32),
            pltpu.VMEM((32, NODE_DEV), I32),
            pltpu.VMEM((3, NODE_DEV), F32),
            pltpu.VMEM((8, NODE_DEV), F32),
            pltpu.VMEM((LANES, NODE_DEV), BF16),
            pltpu.VMEM((16, LANES), I32),
            pltpu.VMEM((8, NODE_DEV), F32),
            pltpu.VMEM((8, WIN), F32),
            pltpu.VMEM((8, WIN), F32),
            pltpu.VMEM((3, WIDE * LANES), F32),
            pltpu.VMEM((3, WIDE * LANES), F32),
            pltpu.VMEM((3, WIDE * LANES), F32),
            pltpu.VMEM((4, LANES), F32),
            pltpu.VMEM((DEVICES, 1, LANES), F32),
            pltpu.VMEM((DEVICES, 1, LANES), F32),
            pltpu.VMEM((4, CROWS, LANES), F32),
            pltpu.VMEM((3, CROWS, LANES), F32),
            pltpu.VMEM((3, LANES, LANES), F32),
            pltpu.VMEM((GROUPS, 96, LANES), F32),
            pltpu.VMEM((9, 32, 2 * LANES), F32),
            pltpu.VMEM((32, 2 * LANES), I32),
            pltpu.VMEM((CROWS, LANES), I32),
            pltpu.VMEM((CUBE, 8, LANES), F32),
            pltpu.VMEM((CSWEEPS, CUBE, 8, LANES), F32),
            dma((9,)),
            dma((3, 2)),
            dma((3, 2)),
            pltpu.SemaphoreType.REGULAR((3,)),
            dma((3,)),
            dma((3,)),
            dma((3,)),
            dma((3,)),
            dma((CSWEEPS - 1,)),
            dma((CSWEEPS - 1, CUBE)),
        ],
        compiler_params=pltpu.CompilerParams(collective_id=0, has_side_effects=True),
        name="vcycle",
    )(
        b.T,
        d.T,
        q.T,
        a.transpose(2, 3, 1, 0),
        agg.reshape(BLOCKS, LANES),
        row.reshape(1, AGG_DEV),
        cd.T,
        cq,
        ca.transpose(2, 3, 0, 1),
    )
    sol, cor = pl.pallas_call(
        split,
        out_shape=(
            jax.ShapeDtypeStruct((3, NODE_DEV), F32),
            jax.ShapeDtypeStruct((3, AGG_DEV), F32),
        ),
        in_specs=[vmem],
        out_specs=(vmem, vmem),
        name="split",
    )(pltpu.with_memory_space_constraint(out, pltpu.VMEM))
    return sol.T, cor.T


def solution(mesh):
    rows, line = P("dom", None), P("dom")
    blocks = P("dom", None, None, None)
    return jax.shard_map(
        body,
        mesh=mesh,
        in_specs=(rows, rows, rows, blocks, line, line, rows, rows, blocks),
        out_specs=(rows, rows),
        check_vma=False,
    )
```
